128 devices in a mesh: rep: 2 (over core), dp: 64 (over x, y, z).
Axes of the slice: x: 4, y: 4, z: 4, core: 2. Of those that a mesh axis runs over, the one named last changes fastest.
Arguments:
- x: bfloat16 [128, 2048, 1024], P(('rep', 'dp')), parts along dimension 0
- dy: bfloat16 [128, 2048, 1024], P(('rep', 'dp')), parts along dimension 0
- w_gate: bfloat16 [2, 1024, 2816], replicated
- w_up: bfloat16 [2, 1024, 2816], replicated
- w_down: bfloat16 [2, 2816, 1024], replicated
- m_w_gate: float32 [2, 1024, 2816], P(None, 'dp')
- m_w_up: float32 [2, 1024, 2816], P(None, 'dp')
- m_w_down: float32 [2, 2816, 1024], P(None, 'dp')
- v_w_gate: float32 [2, 1024, 2816], P(None, 'dp')
- v_w_up: float32 [2, 1024, 2816], P(None, 'dp')
- v_w_down: float32 [2, 2816, 1024], P(None, 'dp')
Outputs:
- output 1: bfloat16 [4, 1024, 2816], P('rep'), parts along dimension 0
- output 2: bfloat16 [4, 1024, 2816], P('rep'), parts along dimension 0
- output 3: bfloat16 [4, 2816, 1024], P('rep'), parts along dimension 0
- output 4: float32 [4, 1024, 2816], P('rep', 'dp'), parts along dimension 0
- output 5: float32 [4, 1024, 2816], P('rep', 'dp'), parts along dimension 0
- output 6: float32 [4, 2816, 1024], P('rep', 'dp'), parts along dimension 0
- output 7: float32 [4, 1024, 2816], P('rep', 'dp'), parts along dimension 0
- output 8: float32 [4, 1024, 2816], P('rep', 'dp'), parts along dimension 0
- output 9: float32 [4, 2816, 1024], P('rep', 'dp'), parts along dimension 0
There are 2 independent parts. The reference program is written for one: setup_inputs(seed, part) draws one part's arguments, and reference() takes and returns one part's arrays. A program takes and returns all parts, laid end to end along the dimension named above; an argument that names none is the same for every part.
All inputs are finite; a program needn't handle non-finite values.
Results may differ from the reference program's by a relative error of at most 0.022.
Values are sent between devices in bfloat16 or wider.
A program may use at most 1.5 GiB of HBM per device.

```python
import jax
import jax.numpy as jnp
from jax import lax

SEQUENCES = 64
TOKENS = 2048
D = 1024
FF = 2816
LAYERS = 2
NAMES = ("w_gate", "w_up", "w_down")
SHAPES = {"w_gate": (LAYERS, D, FF), "w_up": (LAYERS, D, FF), "w_down": (LAYERS, FF, D)}


def bump(key, n, height):
    away = (jnp.arange(n, dtype=jnp.int32) - jax.random.randint(key, (), 0, n, jnp.int32)) % n
    return jnp.where(away < n // 8, height, 1.0)


def together(key, own, strength):
    shared = jax.random.normal(key, own.shape[1:], jnp.float32)
    return (own + strength * shared) * lax.rsqrt(1 + strength * strength)


def setup_inputs(seed: int = 0, part: int = 0) -> dict:
    kx, kdy, ka, kb, kz, kf, kh, kl, *keys = jax.random.split(jax.random.key(seed), 8 + 3 * len(NAMES))
    kx, kdy, ka, kb = (jax.random.fold_in(k, part) for k in (kx, kdy, ka, kb))
    kw, km, kv = (keys[i::3] for i in range(3))
    shape = (SEQUENCES, TOKENS, D)
    much_x, much_dy = jax.random.uniform(kz, (2,), jnp.float32, 0.0, 1.0)
    loud = 2.0 ** jax.random.uniform(jax.random.fold_in(kz, 1), (), jnp.float32, -1.0, 2.0)
    layers = 2.0 ** jax.random.uniform(kl, (LAYERS, 1, 1), jnp.float32, -1.0, 1.0)
    x = together(ka, jax.random.normal(kx, shape, jnp.float32), much_x) * bump(kf, D, 4.0)
    dy = together(kb, jax.random.normal(kdy, shape, jnp.float32), much_dy)
    drawn = {"x": x.astype(jnp.bfloat16), "dy": (loud * dy * (SEQUENCES * TOKENS) ** -0.5).astype(jnp.bfloat16)}
    for key, name in zip(kw, NAMES, strict=True):
        w = jax.random.normal(key, SHAPES[name], jnp.float32) * SHAPES[name][1] ** -0.5
        drawn[name] = (w * {"w_gate": 1.0, "w_up": bump(kh, FF, 4.0), "w_down": layers}[name]).astype(jnp.bfloat16)
    for key, name in zip(km, NAMES, strict=True):
        drawn[f"m_{name}"] = 0.1 * jax.random.normal(key, SHAPES[name], jnp.float32)
    for key, name in zip(kv, NAMES, strict=True):
        drawn[f"v_{name}"] = jax.random.uniform(key, SHAPES[name], jnp.float32, 0.005, 0.015)
    return drawn


def matmul(a, w):
    return jnp.dot(a, w, preferred_element_type=jnp.float32).astype(jnp.bfloat16)


def normed(h):
    wide = h.astype(jnp.float32)
    scale = lax.rsqrt(jnp.mean(wide**2, -1, keepdims=True) + 1e-6)
    return (wide * scale).astype(jnp.bfloat16)


def layer(h, w):
    a = normed(h)
    gate = jnp.dot(a, w["w_gate"], preferred_element_type=jnp.float32)
    up = jnp.dot(a, w["w_up"], preferred_element_type=jnp.float32)
    return h + matmul((jax.nn.silu(gate) * up).astype(jnp.bfloat16), w["w_down"])


def adamw(w, m, v, g):
    m = 0.9 * m + 0.1 * g
    v = 0.95 * v + 0.05 * g * g
    step = m * lax.rsqrt(v + 1e-8) + 0.1 * w
    return (w - 0.02 * step).astype(jnp.bfloat16), m, v


def clipped(gradients, sum_of_squares, count):
    factor = jnp.minimum(1.0, 0.5 * lax.rsqrt(sum_of_squares / count + 1e-30))
    return [g * factor for g in gradients]


def stack(weights, h):
    return lax.scan(lambda h, w: (layer(h, w), None), h, weights)[0]


def reference(x, dy, w_gate, w_up, w_down, m_w_gate, m_w_up, m_w_down, v_w_gate, v_w_up, v_w_down):
    weights = dict(zip(NAMES, (w_gate, w_up, w_down), strict=True))

    def take(so_far, sequence):
        h, by_y = sequence
        _, back = jax.vjp(lambda w: stack(w, h), weights)
        return jax.tree.map(lambda total, term: total + term.astype(jnp.float32), so_far, back(by_y)[0]), None

    none_yet = {name: jnp.zeros(w.shape, jnp.float32) for name, w in weights.items()}
    by_weights, _ = lax.scan(take, none_yet, (x, dy))
    gradients = [by_weights[name].astype(jnp.bfloat16).astype(jnp.float32) for name in NAMES]
    gradients = clipped(gradients, sum(jnp.sum(g * g) for g in gradients), sum(g.size for g in gradients))
    new = [
        adamw(w.astype(jnp.float32), m, v, g)
        for w, m, v, g in zip((w_gate, w_up, w_down), (m_w_gate, m_w_up, m_w_down), (v_w_gate, v_w_up, v_w_down), gradients, strict=True)
    ]
    return tuple(one[which] for which in range(3) for one in new)
```

```python
import jax
import jax.numpy as jnp
from jax import lax
from jax.experimental import pallas as pl
from jax.experimental.pallas import tpu as pltpu
from jax.sharding import PartitionSpec as P

NAMES = ("w_gate", "w_up", "w_down")
BF16, F32 = jnp.bfloat16, jnp.float32
MESH = pl.DeviceIdType.MESH
VMEM_LIMIT = 63 * 1024 * 1024
WIDE, DEEP = "wide", "deep"
ROWS = {WIDE: 64, DEEP: 176}
WINDOW = {WIDE: 16, DEEP: 48}
COLUMNS = {WIDE: 2816, DEEP: 1024}
JOBS = {
    WIDE: ((0, 1, 0, 512), (0, -1, 512, 384), (1, 1, 896, 384), (1, -1, 1280, 512), (2, 1, 1792, 512), (2, -1, 2304, 512)),
    DEEP: ((0, 1, 0, 256), (0, -1, 256, 128), (1, 1, 384, 128), (1, -1, 512, 256), (2, 1, 768, 128), (2, -1, 896, 128)),
}
COLOURS = {
    WIDE: ((0, 0, 896), (1, 896, 896), (2, 1792, 1024)),
    DEEP: ((0, 0, 384), (1, 384, 384), (2, 768, 256)),
}


def coordinates():
    i = lax.axis_index("dp")
    return [lax.div(i, 16), lax.rem(lax.div(i, 4), 4), lax.rem(i, 4)]


def at(axis, by):
    c = coordinates()
    c[axis] = lax.rem(c[axis] + by + 4, 4)
    return {"dp": c[0] * 16 + c[1] * 4 + c[2]}


def place(axis, by):
    return lax.rem(coordinates()[axis] + by + 4, 4)


def greet(offsets):
    barrier = pltpu.get_barrier_semaphore()
    for axis, by in offsets:
        pl.semaphore_signal(barrier, inc=1, device_id=at(axis, by), device_id_type=MESH)
    pl.semaphore_wait(barrier, len(offsets))


NEXT = tuple((axis, by) for axis in range(3) for by in (1, -1))


def first_row(form, z):
    if form == WIDE:
        return pl.multiple_of(z * 16, 8)
    return pl.multiple_of(lax.div(z, 2) * 88 + lax.rem(z, 2) * 40, 8)


def part(form, axis, k):
    index = [slice(None)] * 3
    index[axis] = pl.ds(first_row(form, k), WINDOW[form]) if axis == 2 else pl.ds(k, 1)
    return tuple(index)


def extent(form, done):
    return (1 if 0 in done else 4, 1 if 1 in done else 4, WINDOW[form] if 2 in done else ROWS[form])


class Scratch:
    def __init__(self):
        self.shapes = []

    def new(self, shape, dtype):
        self.shapes.append(pltpu.VMEM(shape, dtype))
        return len(self.shapes) - 1


class Copies:
    def __init__(self):
        self.count = 0

    def new(self):
        self.count += 1
        return self.count - 1


def each(shape, body):
    def step(t, _):
        body(lax.div(t, shape[1]), lax.rem(t, shape[1]))
        return 0

    lax.fori_loop(0, shape[0] * shape[1], step, 0)


class SumJob:
    def __init__(self, form, job, scratch, remote, local):
        self.form = form
        self.colour, self.d, self.first, self.width = job
        self.axes = [(self.colour + n) % 3 for n in range(3)]
        done = []
        self.phases = []
        for n, axis in enumerate(self.axes):
            done.append(axis)
            shape = (*extent(form, done), self.width)
            names = {}
            for name in ("r1", "ro", "rm", "sm"):
                names[name] = scratch.new(shape, BF16)
            if n == 0:
                names["own"] = scratch.new(shape, BF16)
                names["l1"], names["l0"] = local.new(), local.new()
            else:
                names["s1"] = scratch.new(shape, BF16)
                names["so"] = scratch.new(shape, BF16)
            if n < 2:
                names["acc"] = scratch.new(shape, F32)
            for name in ("c1", "co", "cm"):
                names[name] = remote.new()
            self.phases.append((axis, shape, names))

    def bind(self, source, out, squares, refs, send, recv, local):
        self.source, self.out, self.squares = source, out, squares
        self.refs, self.send, self.recv, self.local = refs, send, recv, local

    def buf(self, n, name):
        return self.refs[self.phases[n][2][name]]

    def copy(self, n, which):
        axis, _, names = self.phases[n]
        d = self.d
        target, by = {"c1": ("r1", d), "co": ("ro", -d), "cm": ("rm", d)}[which]
        if which == "cm":
            source = self.buf(n, "sm")
        elif n == 0:
            k = place(axis, 2 if which == "c1" else -d)
            source = self.source.at[(*part(self.form, axis, k), pl.ds(self.first, self.width))]
        else:
            source = self.buf(n, "s1" if which == "c1" else "so")
        number = names[which]
        return pltpu.make_async_remote_copy(
            src_ref=source,
            dst_ref=self.buf(n, target),
            send_sem=self.send.at[number],
            recv_sem=self.recv.at[number],
            device_id=at(axis, by),
            device_id_type=MESH,
        )

    def load(self, which):
        axis, _, names = self.phases[0]
        k = place(axis, self.d if which == "l1" else 0)
        return pltpu.make_async_copy(
            self.source.at[(*part(self.form, axis, k), pl.ds(self.first, self.width))],
            self.buf(0, "sm" if which == "l1" else "own"),
            self.local.at[names[which]],
        )

    def rows(self, n, k):
        axis = self.phases[n][0]
        acc = self.buf(n - 1, "acc")

        def read(i, j):
            if axis == 0:
                return acc[k, j]
            if axis == 1:
                return acc[i, k]
            return acc[i, j, pl.ds(first_row(self.form, k), WINDOW[self.form]), :]

        return read

    def begin(self, n):
        axis, shape, _ = self.phases[n]
        if n == 0:
            self.copy(0, "c1").start()
            self.load("l1").start()
            self.copy(0, "co").start()
            self.load("l0").start()
            return
        for name, by, copy in (("s1", 2, "c1"), ("so", -self.d, "co")):
            read, buf = self.rows(n, place(axis, by)), self.buf(n, name)

            def body(i, j):
                buf[i, j] = read(i, j).astype(BF16)

            each(shape, body)
            self.copy(n, copy).start()

    def middle(self, n):
        axis, shape, _ = self.phases[n]
        r1, sm = self.buf(n, "r1"), self.buf(n, "sm")
        if n == 0:
            self.load("l1").wait()
            read = lambda i, j: sm[i, j].astype(F32)
        else:
            read = self.rows(n, place(axis, self.d))
        self.copy(n, "c1").wait_recv()

        def body(i, j):
            sm[i, j] = (read(i, j) + r1[i, j].astype(F32)).astype(BF16)

        each(shape, body)
        self.copy(n, "cm").start()

    def end(self, n):
        axis, shape, _ = self.phases[n]
        rm, ro = self.buf(n, "rm"), self.buf(n, "ro")
        if n == 0:
            self.load("l0").wait()
            own = self.buf(0, "own")
            read = lambda i, j: own[i, j].astype(F32)
        else:
            read = self.rows(n, place(axis, 0))
        self.copy(n, "co").wait_recv()
        self.copy(n, "cm").wait_recv()

        def total(i, j):
            return read(i, j) + rm[i, j].astype(F32) + ro[i, j].astype(F32)

        if n < 2:
            acc = self.buf(n, "acc")

            def body(i, j):
                acc[i, j] = total(i, j)

            each(shape, body)
            return
        g = total(0, 0).astype(BF16)
        self.out[:, pl.ds(self.first, self.width)] = g
        square = g.astype(F32)
        square = square * square
        if self.form == DEEP:
            row = lax.broadcasted_iota(jnp.int32, square.shape, 0) - 4 * lax.rem(coordinates()[2], 2)
            square = jnp.where((row >= 0) & (row < 44), square, 0.0)
        square = jnp.sum(square, axis=0, keepdims=True)
        for t in range(self.width // 128):
            self.squares[...] += square[:, 128 * t : 128 * (t + 1)]

    def sent(self):
        for n in range(3):
            for which in ("c1", "co", "cm"):
                self.copy(n, which).wait_send()

    def actions(self):
        yield lambda: self.begin(0)
        yield lambda: self.middle(0)
        for n in (1, 2):

            def turn(n=n):
                self.end(n - 1)
                self.begin(n)

            yield turn
            yield lambda n=n: self.middle(n)

        def last():
            self.end(2)
            self.sent()

        yield last


def sum_kernel(forms, number):
    scratch, remote, local = Scratch(), Copies(), Copies()
    jobs = [[SumJob(form, job, scratch, remote, local) for job in JOBS[form]] for form in forms]

    def kernel(*refs):
        sources, refs = refs[: len(forms)], refs[len(forms) :]
        outs, squares, refs = refs[: len(forms)], refs[len(forms)], refs[len(forms) + 1 :]
        send, recv, loc = refs[-3:]
        greet(NEXT)
        squares[...] = jnp.zeros_like(squares)
        order = []
        for m, of_matrix in enumerate(jobs):
            for j, job in enumerate(of_matrix):
                job.bind(sources[m], outs[m], squares, refs[:-3], send, recv, loc)
                for stage, action in enumerate(job.actions()):
                    order.append((stage + 1.5 * m, m, stage, j, action))
        for *_, action in sorted(order, key=lambda o: o[:4]):
            action()

    def call(*terms):
        *sums, squares = pl.pallas_call(
            kernel,
            out_shape=[jax.ShapeDtypeStruct((WINDOW[f], COLUMNS[f]), BF16) for f in forms] + [jax.ShapeDtypeStruct((1, 128), F32)],
            in_specs=[pl.BlockSpec(memory_space=pl.ANY)] * len(forms),
            out_specs=[pl.BlockSpec(memory_space=pltpu.VMEM)] * (len(forms) + 1),
            scratch_shapes=[
                *scratch.shapes,
                pltpu.SemaphoreType.DMA((remote.count,)),
                pltpu.SemaphoreType.DMA((remote.count,)),
                pltpu.SemaphoreType.DMA((local.count,)),
            ],
            compiler_params=pltpu.CompilerParams(collective_id=number, has_side_effects=True, vmem_limit_bytes=VMEM_LIMIT),
            name=f"sum_{number}",
        )(*(t.reshape(4, 4, ROWS[f], COLUMNS[f]) for t, f in zip(terms, forms, strict=True)))
        return sums, squares

    return call


def norm_kernel(number):
    around = (1, -1, 2)

    def kernel(own, out, got, total, send, recv):
        greet(tuple((axis, by) for axis in range(3) for by in around))
        total[0] = own[...]
        for axis in range(3):
            copies = [
                pltpu.make_async_remote_copy(
                    src_ref=total.at[axis],
                    dst_ref=got.at[axis, n],
                    send_sem=send.at[axis, n],
                    recv_sem=recv.at[axis, n],
                    device_id=at(axis, by),
                    device_id_type=MESH,
                )
                for n, by in enumerate(around)
            ]
            for copy in copies:
                copy.start()
            for copy in copies:
                copy.wait_recv()
            total[axis + 1] = (total[axis] + got[axis, 2]) + (got[axis, 0] + got[axis, 1])
            for copy in copies:
                copy.wait_send()
        out[...] = total[3]

    return pl.pallas_call(
        kernel,
        out_shape=jax.ShapeDtypeStruct((8, 128), F32),
        in_specs=[pl.BlockSpec(memory_space=pltpu.VMEM)],
        out_specs=pl.BlockSpec(memory_space=pltpu.VMEM),
        scratch_shapes=[
            pltpu.VMEM((3, 3, 8, 128), F32),
            pltpu.VMEM((4, 8, 128), F32),
            pltpu.SemaphoreType.DMA((3, 3)),
            pltpu.SemaphoreType.DMA((3, 3)),
        ],
        compiler_params=pltpu.CompilerParams(collective_id=number, has_side_effects=True),
        name="norm",
    )


class GatherJob:
    def __init__(self, form, colour, remote, local):
        self.form = form
        self.colour, self.first, self.width = colour
        self.axes = [(self.colour + n) % 3 for n in range(3)]
        self.numbers = [[remote.new() for _ in range(4)] for _ in range(3)]
        self.local_number = local.new()

    def bind(self, own, out, send, recv, local):
        self.own, self.out, self.send, self.recv, self.local = own, out, send, recv, local

    def held(self, n, by, layer=None):
        index = []
        for axis in range(3):
            if axis in self.axes[:n]:
                index.append(slice(None))
                continue
            k = place(axis, by if axis == self.axes[n] else 0)
            window = WINDOW[self.form]
            index.append(pl.ds(pl.multiple_of(k * window, 8), window) if axis == 2 else pl.ds(k, 1))
        layers = slice(None) if layer is None else pl.ds(layer, 1)
        return self.out.at[(layers, *index, pl.ds(self.first, self.width))]

    def copy(self, n, which):
        axis, number = self.axes[n], self.numbers[n][which]
        if which < 2:
            by = (1, -1)[which]
            source = self.own.at[:, :, :, :, pl.ds(self.first, self.width)] if n == 0 else self.held(n, 0)
            target = self.held(n, 0)
        else:
            by = (1, -1)[which - 2]
            source = target = self.held(n, -by, which - 2)
        return pltpu.make_async_remote_copy(
            src_ref=source,
            dst_ref=target,
            send_sem=self.send.at[number],
            recv_sem=self.recv.at[number],
            device_id=at(axis, by),
            device_id_type=MESH,
        )

    def keep(self):
        return pltpu.make_async_copy(
            self.own.at[:, :, :, :, pl.ds(self.first, self.width)], self.held(0, 0), self.local.at[self.local_number]
        )

    def actions(self):
        for n in range(3):

            def begin(n=n):
                if n == 0:
                    self.keep().start()
                else:
                    self.copy(n - 1, 2).wait_recv()
                    self.copy(n - 1, 3).wait_recv()
                if n == 1:
                    self.keep().wait()
                self.copy(n, 0).start()
                self.copy(n, 1).start()

            def forward(n=n):
                self.copy(n, 0).wait_recv()
                self.copy(n, 2).start()
                self.copy(n, 1).wait_recv()
                self.copy(n, 3).start()

            yield begin
            yield forward

        def last():
            self.copy(2, 2).wait_recv()
            self.copy(2, 3).wait_recv()
            for n in range(3):
                for which in range(4):
                    self.copy(n, which).wait_send()

        yield last


def gather_kernel(forms, number):
    remote, local = Copies(), Copies()
    jobs = [[GatherJob(form, colour, remote, local) for colour in COLOURS[form]] for form in forms]

    def kernel(*refs):
        owns, outs = refs[: len(forms)], refs[len(forms) : 2 * len(forms)]
        send, recv, loc = refs[2 * len(forms) :]
        greet(NEXT)
        order = []
        for m, of_matrix in enumerate(jobs):
            for j, job in enumerate(of_matrix):
                job.bind(owns[m], outs[m], send, recv, loc)
                for stage, action in enumerate(job.actions()):
                    order.append((stage, m, j, action))
        for *_, action in sorted(order, key=lambda o: o[:3]):
            action()

    def call(*owns):
        return pl.pallas_call(
            kernel,
            out_shape=[jax.ShapeDtypeStruct((2, 4, 4, 4 * WINDOW[f], COLUMNS[f]), BF16) for f in forms],
            in_specs=[pl.BlockSpec(memory_space=pltpu.VMEM)] * len(forms),
            out_specs=[pl.BlockSpec(memory_space=pl.ANY)] * len(forms),
            scratch_shapes=[
                pltpu.SemaphoreType.DMA((remote.count,)),
                pltpu.SemaphoreType.DMA((remote.count,)),
                pltpu.SemaphoreType.DMA((local.count,)),
            ],
            compiler_params=pltpu.CompilerParams(collective_id=number, has_side_effects=True),
            name="gather",
        )(*(o.reshape(2, 1, 1, WINDOW[f], COLUMNS[f]) for o, f in zip(owns, forms, strict=True)))

    return call


def matmul(a, w):
    return jnp.dot(a, w, preferred_element_type=F32).astype(BF16)


def normed(h):
    wide = h.astype(F32)
    scale = lax.rsqrt(jnp.mean(wide**2, -1, keepdims=True) + 1e-6)
    return (wide * scale).astype(BF16)


def layer(h, w):
    a = normed(h)
    gate = jnp.dot(a, w["w_gate"], preferred_element_type=F32)
    up = jnp.dot(a, w["w_up"], preferred_element_type=F32)
    return h + matmul((jax.nn.silu(gate) * up).astype(BF16), w["w_down"])


def adamw(w, m, v, g):
    m = 0.9 * m + 0.1 * g
    v = 0.95 * v + 0.05 * g * g
    step = m * lax.rsqrt(v + 1e-8) + 0.1 * w
    return (w - 0.02 * step).astype(BF16), m, v


def stack(weights, h):
    for w in weights:
        h = layer(h, w)
    return h


def solution(mesh):
    def step(x, dy, *arrays):
        weights, m, v = (arrays[i : i + 3] for i in (0, 3, 6))
        x, dy = x[0], dy[0]
        by_layer = [{name: w[n] for name, w in zip(NAMES, weights, strict=True)} for n in range(2)]
        _, back = jax.vjp(lambda w: stack(w, x), by_layer)
        terms = back(dy)[0]
        z = lax.rem(lax.axis_index("dp"), 4)
        gate, up, down, squares = [None] * 2, [None] * 2, [None] * 2, []
        (down[1], down[0]), s = sum_kernel((DEEP, DEEP), 0)(terms[1]["w_down"], terms[0]["w_down"])
        squares.append(s)
        for n in (1, 0):
            (gate[n], up[n]), s = sum_kernel((WIDE, WIDE), 1 + n)(terms[n]["w_gate"], terms[n]["w_up"])
            squares.append(s)
        down = [lax.dynamic_slice_in_dim(d, 4 * lax.rem(z, 2), 44, 0) for d in down]
        gradients = [jnp.stack(g).astype(F32) for g in (gate, up, down)]
        squares = jnp.broadcast_to(sum(jnp.sum(s) for s in squares), (8, 128))
        total = norm_kernel(3)(squares)[0, 0]
        factor = jnp.minimum(1.0, 0.5 * lax.rsqrt(total / (6 * 1024 * 2816) + 1e-30))
        new = []
        for w, m_, v_, g in zip(weights, m, v, gradients, strict=True):
            rows = g.shape[1]
            own = lax.dynamic_slice_in_dim(w, lax.axis_index("dp") * rows, rows, 1)
            new.append(adamw(own.astype(F32), m_, v_, g * factor))
        own = [one[0] for one in new]
        own[2] = jnp.pad(own[2], ((0, 0), (0, 4), (0, 0)))
        gate, up, down = gather_kernel((WIDE, WIDE, DEEP), 4)(*own)
        down = down.reshape(2, 64, 48, 1024)[:, :, :44].reshape(2, 2816, 1024)
        return (
            gate.reshape(2, 1024, 2816),
            up.reshape(2, 1024, 2816),
            down,
            *(one[1] for one in new),
            *(one[2] for one in new),
        )

    whole, rows = P(None, None, None), P(None, "dp", None)
    tokens, out, out_rows = P(("rep", "dp"), None, None), P("rep", None, None), P("rep", "dp", None)
    return jax.shard_map(
        step,
        mesh=mesh,
        in_specs=(tokens, tokens, *[whole] * 3, *[rows] * 6),
        out_specs=(*[out] * 3, *[out_rows] * 6),
        check_vma=False,
    )
```

```python
import functools

import jax
import jax.numpy as jnp
from jax import lax
from jax.experimental import pallas as pl
from jax.experimental.pallas import tpu as pltpu
from jax.sharding import PartitionSpec as P

NAMES = ("w_gate", "w_up", "w_down")
AXES = range(3)
PAIR = pltpu.SemaphoreType.DMA((2,))
BF16, F32 = jnp.bfloat16, jnp.float32
MESH = pl.DeviceIdType.MESH
VMEM_LIMIT, SMALL_LIMIT = 63 << 20, 8 << 20
TOKENS, D, FF = 2048, 1024, 2816
WIDE, DEEP = "wide", "deep"
ROWS = {WIDE: 64, DEEP: 176}
WINDOW = {WIDE: 16, DEEP: 48}
COLUMNS = {WIDE: FF, DEEP: D}
TILE = 256
TILES = FF // TILE
GATE = tuple((n % 3, 1 - 2 * (n // 3 % 2), TILE * (n + min(n, 4)), 2 * TILE if n < 4 else TILE) for n in range(7))
UP = tuple(((c + 1) % 3, -d, first, width) for c, d, first, width in GATE)
DOWN = ((0, 1, 0, 256), (0, -1, 256, 128), (1, 1, 384, 128), (1, -1, 512, 128), (2, 1, 640, 128), (2, -1, 768, 256))
SECOND_DOWN, SECOND_WIDE = (0, 5, 12, 18, 20, 26, 82), (0, 6, 10, 13, 27, 36, 77)
FIRST_DOWN, FIRST_WIDE = (0, 5, 10, 13, 18, 20, 32), (0, 3, 6, 9, 12, 22, 39)
READY = (2, 4, 6, 8, 9, 10, 11)
COLOURS = {
    WIDE: ((0, 0, 896), (1, 896, 896), (2, 1792, 1024)),
    DEEP: ((0, 0, 384), (1, 384, 384), (2, 768, 256)),
}


def coordinates():
    i = lax.axis_index("dp")
    return [lax.div(i, 16), lax.rem(lax.div(i, 4), 4), lax.rem(i, 4)]


def at(axis, by):
    c = coordinates()
    c[axis] = lax.rem(c[axis] + by + 4, 4)
    return {"dp": c[0] * 16 + c[1] * 4 + c[2]}


def place(axis, by):
    return lax.rem(coordinates()[axis] + by + 4, 4)


def greet(offsets):
    barrier = pltpu.get_barrier_semaphore()
    for axis, by in offsets:
        pl.semaphore_signal(barrier, inc=1, device_id=at(axis, by), device_id_type=MESH)
    pl.semaphore_wait(barrier, len(offsets))


NEXT = tuple((axis, by) for axis in AXES for by in (1, -1))


def first_row(form, z):
    if form == WIDE:
        return pl.multiple_of(z * 16, 8)
    return pl.multiple_of(lax.div(z, 2) * 88 + lax.rem(z, 2) * 40, 8)


def part(form, axis, k):
    index = [slice(None)] * 3
    index[axis] = pl.ds(first_row(form, k), WINDOW[form]) if axis == 2 else pl.ds(k, 1)
    return tuple(index)


def extent(form, done):
    return (1 if 0 in done else 4, 1 if 1 in done else 4, WINDOW[form] if 2 in done else ROWS[form])


class Scratch:
    def __init__(self):
        self.shapes = []

    def new(self, shape, dtype):
        self.shapes.append(pltpu.VMEM(shape, dtype))
        return len(self.shapes) - 1


class Copies:
    def __init__(self):
        self.count = 0

    def new(self):
        self.count += 1
        return self.count - 1


def each(shape, body):
    def step(t, _):
        body(lax.div(t, shape[1]), lax.rem(t, shape[1]))
        return 0

    lax.fori_loop(0, shape[0] * shape[1], step, 0)


class SumJob:
    def __init__(self, form, job, scratch, remote, local):
        self.form = form
        self.colour, self.d, self.first, self.width = job
        self.axes = [(self.colour + n) % 3 for n in AXES]
        done = []
        self.phases = []
        for n, axis in enumerate(self.axes):
            done.append(axis)
            shape = (*extent(form, done), self.width)
            names = {}
            for name in ("r1", "ro", "rm", "sm"):
                names[name] = scratch.new(shape, BF16)
            if n == 0:
                names["l1"], names["l0"] = local.new(), local.new()
            else:
                names["s1"] = scratch.new(shape, BF16)
                names["so"] = scratch.new(shape, BF16)
            if n < 2:
                names["acc"] = scratch.new(shape, F32)
            for name in ("c1", "co", "cm"):
                names[name] = remote.new()
            self.phases.append((axis, shape, names))

    def bind(self, source, out, squares, refs, send, recv, local):
        self.source, self.out, self.squares = source, out, squares
        self.refs, self.send, self.recv, self.local = refs, send, recv, local

    def buf(self, n, name):
        return self.refs[self.phases[n][2][name]]

    def copy(self, n, which):
        axis, _, names = self.phases[n]
        d = self.d
        target, by = {"c1": ("r1", d), "co": ("ro", -d), "cm": ("rm", d)}[which]
        if which == "cm":
            source = self.buf(n, "sm")
        elif n == 0:
            k = place(axis, 2 if which == "c1" else -d)
            source = self.source.at[(*part(self.form, axis, k), pl.ds(self.first, self.width))]
        else:
            source = self.buf(n, "s1" if which == "c1" else "so")
        number = names[which]
        return pltpu.make_async_remote_copy(
            src_ref=source,
            dst_ref=self.buf(n, target),
            send_sem=self.send.at[number],
            recv_sem=self.recv.at[number],
            device_id=at(axis, by),
            device_id_type=MESH,
        )

    def load(self, which):
        axis, _, names = self.phases[0]
        k = place(axis, self.d if which == "l1" else 0)
        return pltpu.make_async_copy(
            self.source.at[(*part(self.form, axis, k), pl.ds(self.first, self.width))],
            self.buf(0, "sm" if which == "l1" else "r1"),
            self.local.at[names[which]],
        )

    def rows(self, n, k):
        axis = self.phases[n][0]
        acc = self.buf(n - 1, "acc")

        def read(i, j):
            if axis == 0:
                return acc[k, j]
            if axis == 1:
                return acc[i, k]
            return acc[i, j, pl.ds(first_row(self.form, k), WINDOW[self.form]), :]

        return read

    def begin(self, n):
        axis, shape, _ = self.phases[n]
        if n == 0:
            self.copy(0, "c1").start()
            self.load("l1").start()
            self.copy(0, "co").start()
            return
        for name, by, copy in (("s1", 2, "c1"), ("so", -self.d, "co")):
            read, buf = self.rows(n, place(axis, by)), self.buf(n, name)

            def body(i, j):
                buf[i, j] = read(i, j).astype(BF16)

            each(shape, body)
            self.copy(n, copy).start()

    def middle(self, n):
        axis, shape, _ = self.phases[n]
        r1, sm = self.buf(n, "r1"), self.buf(n, "sm")
        if n == 0:
            self.load("l1").wait()
            read = lambda i, j: sm[i, j].astype(F32)
        else:
            read = self.rows(n, place(axis, self.d))
        self.copy(n, "c1").wait_recv()

        def body(i, j):
            sm[i, j] = (read(i, j) + r1[i, j].astype(F32)).astype(BF16)

        each(shape, body)
        self.copy(n, "cm").start()
        if n == 0:
            self.load("l0").start()

    def end(self, n):
        axis, shape, _ = self.phases[n]
        rm, ro = self.buf(n, "rm"), self.buf(n, "ro")
        if n == 0:
            self.load("l0").wait()
            own = self.buf(0, "r1")
            read = lambda i, j: own[i, j].astype(F32)
        else:
            read = self.rows(n, place(axis, 0))
        self.copy(n, "co").wait_recv()
        self.copy(n, "cm").wait_recv()

        def total(i, j):
            return read(i, j) + rm[i, j].astype(F32) + ro[i, j].astype(F32)

        if n < 2:
            acc = self.buf(n, "acc")

            def body(i, j):
                acc[i, j] = total(i, j)

            each(shape, body)
            return
        g = total(0, 0).astype(BF16)
        self.out[:, pl.ds(self.first, self.width)] = g
        square = g.astype(F32)
        square = square * square
        if self.form == DEEP:
            row = lax.broadcasted_iota(jnp.int32, square.shape, 0) - 4 * lax.rem(coordinates()[2], 2)
            square = jnp.where((row >= 0) & (row < 44), square, 0.0)
        square = jnp.sum(square, axis=0, keepdims=True)
        for t in range(self.width // 128):
            self.squares[...] += square[:, 128 * t : 128 * (t + 1)]

    def sent(self):
        for n in AXES:
            for which in ("c1", "co", "cm"):
                self.copy(n, which).wait_send()

    def actions(self):
        yield lambda: self.begin(0)
        yield lambda: self.middle(0)
        for n in (1, 2):

            def turn(n=n):
                self.end(n - 1)
                self.begin(n)

            yield turn
            yield lambda n=n: self.middle(n)

        def last():
            self.end(2)
            self.sent()

        yield last


class Sums:
    def __init__(self, matrices):
        self.scratch, self.remote, self.local = Scratch(), Copies(), Copies()
        self.forms = [form for form, *_ in matrices]
        self.jobs = []
        for m, (form, jobs, begins, later) in enumerate(matrices):
            for job, begin in zip(jobs, begins, strict=True):
                self.jobs.append((m, SumJob(form, job, self.scratch, self.remote, self.local), [begin + n for n in later]))
        self.out_shape = [jax.ShapeDtypeStruct((WINDOW[f], COLUMNS[f]), BF16) for f in self.forms]
        self.out_shape.append(jax.ShapeDtypeStruct((1, 128), F32))
        self.scratch_shapes = [
            *self.scratch.shapes,
            pltpu.SemaphoreType.DMA((self.remote.count,)),
            pltpu.SemaphoreType.DMA((self.remote.count,)),
            pltpu.SemaphoreType.DMA((self.local.count,)),
        ]

    def run(self, step, steps, parts, sources, outs, refs):
        *outs, squares = outs
        *refs, send, recv, local = refs
        due, end = {}, steps * parts
        for j, (m, job, times) in enumerate(self.jobs):
            job.bind(sources[m], outs[m], squares, refs, send, recv, local)
            for stage, (time, action) in enumerate(zip(times, job.actions(), strict=True)):
                due.setdefault(min(time, end), []).append((time, stage, j, action))

        def now(time):
            for *_, action in sorted(due.get(time, ()), key=lambda o: o[:3]):
                action()

        def reach(part):
            for time in range(part, end, parts):
                if time in due:
                    pl.when(step == time // parts)(functools.partial(now, time))

        def rest():
            pl.when(step == steps - 1)(functools.partial(now, end))

        def enter(offsets):
            @pl.when(step == 0)
            def _():
                greet(offsets)
                squares[...] = jnp.zeros_like(squares)

        return enter, reach, rest


def dot(a, b, dims=((1,), (0,))):
    return lax.dot_general(a, b, (dims, ((), ())), preferred_element_type=F32)


NT, TN = ((1,), (1,)), ((0,), (0,))
BLOCK = 1024


def blocks(n, size, body):
    lax.fori_loop(0, n // size, lambda t, _: (body(pl.ds(pl.multiple_of(t * size, size), size)), 0)[1], 0)


def kept(shape):
    return pl.BlockSpec(shape, lambda i: (0,) * len(shape), pipeline_mode=pl.Buffered(1))


def wide_tile(number, turn=lambda i: i):
    return pl.BlockSpec((None, D, TILE), lambda i: (number, 0, turn(i)))


def deep_tile(number):
    return pl.BlockSpec((None, TILE, D), lambda i: (number, i, 0))


def columns_tile(turn=lambda i: i):
    return pl.BlockSpec((TOKENS, TILE), lambda i: (0, turn(i)))


ANY = pl.BlockSpec(memory_space=pl.ANY)
VMEM = pl.BlockSpec(memory_space=pltpu.VMEM)


def normed_block(wide):
    return (wide * lax.rsqrt(jnp.mean(wide * wide, -1, keepdims=True) + 1e-6)).astype(BF16)


def first_layer(x, w_gate, w_up, w_down):
    def kernel(x, wg, wu, wd, gate, up, s, a1t, h1, a2, a2t, a_s, h_s, t_s, acc, sem):
        i = pl.program_id(0)

        def put(n, source, target):
            return pltpu.make_async_copy(source, target, sem.at[n])

        @pl.when(i == 0)
        def _():
            def body(rows):
                a = normed_block(x[rows, :].astype(F32))
                a_s[rows, :] = a
                t_s[:, rows] = a.T
                acc[rows, :] = jnp.zeros((TILE, D), F32)

            blocks(TOKENS, TILE, body)
            put(0, t_s, a1t).start()

        def body(rows):
            a = a_s[rows, :]
            g = dot(a, wg[...])
            u = dot(a, wu[...])
            gate[rows, :] = g
            up[rows, :] = u
            p = (g * lax.logistic(g) * u).astype(BF16)
            s[rows, :] = p
            acc[rows, :] += dot(p, wd[...])

        blocks(TOKENS, BLOCK, body)

        @pl.when(i == TILES - 1)
        def _():
            put(0, t_s, a1t).wait()

            def body(rows):
                h = x[rows, :] + acc[rows, :].astype(BF16)
                h_s[rows, :] = h
                a = normed_block(h.astype(F32))
                a_s[rows, :] = a
                t_s[:, rows] = a.T

            blocks(TOKENS, TILE, body)
            copies = [put(0, t_s, a2t), put(1, h_s, h1), put(2, a_s, a2)]
            for copy in copies:
                copy.start()
            for copy in copies:
                copy.wait()

    tokens, turned = jax.ShapeDtypeStruct((TOKENS, D), BF16), jax.ShapeDtypeStruct((D, TOKENS), BF16)
    hidden = (TOKENS, FF)
    return pl.pallas_call(
        kernel,
        grid=(TILES,),
        out_shape=[
            jax.ShapeDtypeStruct(hidden, F32),
            jax.ShapeDtypeStruct(hidden, F32),
            jax.ShapeDtypeStruct(hidden, BF16),
            turned,
            tokens,
            tokens,
            turned,
        ],
        in_specs=[kept((TOKENS, D)), wide_tile(0), wide_tile(0), deep_tile(0)],
        out_specs=[columns_tile()] * 3 + [ANY] * 4,
        scratch_shapes=[
            pltpu.VMEM((TOKENS, D), BF16),
            pltpu.VMEM((TOKENS, D), BF16),
            pltpu.VMEM((D, TOKENS), BF16),
            pltpu.VMEM((TOKENS, D), F32),
            pltpu.SemaphoreType.DMA((3,)),
        ],
        compiler_params=pltpu.CompilerParams(vmem_limit_bytes=VMEM_LIMIT),
        name="first_layer",
    )(x, w_gate, w_up, w_down)


def through_product(ds, g, u):
    sig = lax.logistic(g)
    silu = g * sig
    return (ds * u * (sig + silu * (1.0 - sig))).astype(BF16), (ds * silu).astype(BF16)


def second_layer(a2, dy, w_gate, w_up, w_down):
    def kernel(a2, dy, wg, wu, wd, dg, du, dwd, s):
        def body(rows):
            a = a2[rows, :]
            g = dot(a, wg[...])
            u = dot(a, wu[...])
            ds = dot(dy[rows, :], wd[...], NT).astype(BF16).astype(F32)
            s[rows, :] = (g * lax.logistic(g) * u).astype(BF16)
            dg[rows, :], du[rows, :] = through_product(ds, g, u)

        blocks(TOKENS, BLOCK, body)
        dwd[...] = dot(s[...], dy[...], TN).astype(BF16)

    return pl.pallas_call(
        kernel,
        grid=(TILES,),
        out_shape=[jax.ShapeDtypeStruct((TOKENS, FF), BF16)] * 2 + [jax.ShapeDtypeStruct((FF, D), BF16)],
        in_specs=[kept((TOKENS, D))] * 2 + [wide_tile(1), wide_tile(1), deep_tile(1)],
        out_specs=[columns_tile()] * 2 + [pl.BlockSpec((TILE, D), lambda i: (i, 0))],
        scratch_shapes=[pltpu.VMEM((TOKENS, TILE), BF16)],
        compiler_params=pltpu.CompilerParams(vmem_limit_bytes=VMEM_LIMIT),
        name="second_layer",
    )(a2, dy, w_gate, w_up, w_down)


def down_term(s, dy, da2, h1):
    def kernel(s, dy, da2, h1, out, dh, dh_s, sem):
        copy = pltpu.make_async_copy(dh_s, dh, sem)

        @pl.when(pl.program_id(0) == 0)
        def _():
            def body(rows):
                dh_s[rows, :] = through_norm(dy[rows, :], da2[rows, :], h1[rows, :])

            blocks(TOKENS, TILE, body)
            copy.start()

        out[...] = dot(s[...], dh_s[...], TN).astype(BF16)
        pl.when(pl.program_id(0) == TILES - 1)(copy.wait)

    return pl.pallas_call(
        kernel,
        grid=(TILES,),
        out_shape=[jax.ShapeDtypeStruct((FF, D), BF16), jax.ShapeDtypeStruct((TOKENS, D), BF16)],
        in_specs=[columns_tile()] + [kept((TOKENS, D))] * 3,
        out_specs=[pl.BlockSpec((TILE, D), lambda i: (i, 0)), ANY],
        scratch_shapes=[pltpu.VMEM((TOKENS, D), BF16), pltpu.SemaphoreType.DMA(())],
        compiler_params=pltpu.CompilerParams(vmem_limit_bytes=VMEM_LIMIT),
        name="down_term",
    )(s, dy, da2, h1)


def store_terms(at, dg, du, stage_g, stage_u):
    for stage, cotangent in ((stage_g, dg), (stage_u, du)):
        stage[...] = dot(at[...], cotangent[...]).astype(BF16).reshape(stage.shape)


class Terms:
    def __init__(self, stages, terms, sem):
        self.stages, self.terms, self.sem = stages, terms, sem

    def copies(self, tile):
        columns = pl.ds(pl.multiple_of(tile * TILE, TILE), TILE)
        return [
            pltpu.make_async_copy(stage, term.at[:, :, :, columns], self.sem.at[n])
            for n, (stage, term) in enumerate(zip(self.stages, self.terms, strict=True))
        ]

    def start(self, tile):
        for copy in self.copies(tile):
            copy.start()

    def wait(self, tile):
        for copy in self.copies(tile):
            copy.wait()


TERM = jax.ShapeDtypeStruct((4, 4, 64, FF), BF16)
STAGES = [pltpu.VMEM((4, 4, 64, TILE), BF16)] * 2 + [PAIR]


def second_sums(a2t, dg, du, w_gate, w_up, down, number):
    steps = 2 * TILES
    sums = Sums(
        (
            (DEEP, DOWN, (0,) * 6, SECOND_DOWN),
            (WIDE, GATE, READY, SECOND_WIDE),
            (WIDE, UP, READY, SECOND_WIDE),
        )
    )

    def kernel(a2t, dg, du, wg, wu, down, *refs):
        outs, refs = refs[:4], refs[4:]
        da2, term_g, term_u, stage_g, stage_u, term_sem, acc, half, half_sem, *refs = refs
        i = pl.program_id(0)
        terms = Terms((stage_g, stage_u), (term_g, term_u), term_sem)
        enter, reach, rest = sums.run(i, steps, 1, (down, term_g, term_u), outs, refs)
        enter(NEXT)

        @pl.when((i > 0) & (i <= TILES))
        def _():
            terms.wait(i - 1)

        reach(0)

        @pl.when(i < TILES)
        def _():
            store_terms(a2t, dg, du, stage_g, stage_u)
            terms.start(i)

        @pl.when(i == TILES)
        def _():
            blocks(TOKENS, TILE, lambda rows: acc.__setitem__((rows, slice(None)), jnp.zeros((TILE, D), F32)))

        @pl.when(i >= TILES)
        def _():
            def body(rows):
                acc[rows, :] += dot(dg[rows, :], wg[...], NT) + dot(du[rows, :], wu[...], NT)

            blocks(TOKENS, BLOCK, body)

        @pl.when(i == steps - 1)
        def _():
            for n in range(4):
                rows = pl.ds(512 * n, 512)
                copy = pltpu.make_async_copy(half.at[n % 2], da2.at[rows, :], half_sem.at[n % 2])
                if n >= 2:
                    copy.wait()
                half[n % 2] = acc[rows, :].astype(BF16)
                copy.start()
            for n in (2, 3):
                pltpu.make_async_copy(half.at[n % 2], da2.at[pl.ds(512 * n, 512), :], half_sem.at[n % 2]).wait()

        rest()

    turn = lambda i: lax.rem(i, TILES)
    late = lambda i: jnp.maximum(i - TILES, 0)
    d, g, u, squares, da2, *_ = pl.pallas_call(
        kernel,
        grid=(steps,),
        out_shape=[*sums.out_shape, jax.ShapeDtypeStruct((TOKENS, D), BF16), TERM, TERM],
        in_specs=[kept((D, TOKENS)), columns_tile(turn), columns_tile(turn), wide_tile(1, late), wide_tile(1, late), ANY],
        out_specs=[VMEM] * 4 + [ANY] * 3,
        scratch_shapes=[
            *STAGES,
            pltpu.VMEM((TOKENS, D), F32),
            pltpu.VMEM((2, 512, D), BF16),
            PAIR,
            *sums.scratch_shapes,
        ],
        compiler_params=pltpu.CompilerParams(collective_id=number, has_side_effects=True, vmem_limit_bytes=VMEM_LIMIT),
        name="second_sums",
    )(a2t, dg, du, w_gate, w_up, down.reshape(4, 4, 176, D))
    return d, g, u, squares, da2


def first_sums(a1t, dh, gate, up, w_down, down, others, number):
    steps = TILES
    sums = Sums(
        (
            (DEEP, DOWN, (0,) * 6, FIRST_DOWN),
            (WIDE, GATE, [2 * n for n in READY], FIRST_WIDE),
            (WIDE, UP, [2 * n for n in READY], FIRST_WIDE),
        )
    )

    def kernel(a1t, dh, gate, up, wd, down, others, *refs):
        outs, refs = refs[:4], refs[4:]
        total, term_g, term_u, stage_g, stage_u, term_sem, dg, du, *refs = refs
        *refs, got, held, norm_send, norm_recv = refs
        i = pl.program_id(0)
        terms = Terms((stage_g, stage_u), (term_g, term_u), term_sem)
        enter, reach, rest = sums.run(i, steps, 2, (down, term_g, term_u), outs, refs)
        enter([(axis, by) for axis in AXES for by in AROUND])

        @pl.when(i > 0)
        def _():
            terms.wait(i - 1)

        reach(0)

        def body(rows):
            ds = dot(dh[rows, :], wd[...], NT).astype(BF16).astype(F32)
            dg[rows, :], du[rows, :] = through_product(ds, gate[rows, :], up[rows, :])

        blocks(TOKENS, BLOCK, body)
        reach(1)
        store_terms(a1t, dg, du, stage_g, stage_u)
        terms.start(i)

        @pl.when(i == steps - 1)
        def _():
            terms.wait(i)

        rest()

        @pl.when(i == steps - 1)
        def _():
            norm(jnp.sum(outs[3][...] + others[...]), total, got, held, norm_send, norm_recv)

    d, g, u, _, total, *_ = pl.pallas_call(
        kernel,
        grid=(steps,),
        out_shape=[*sums.out_shape, jax.ShapeDtypeStruct(SCALAR, F32), TERM, TERM],
        in_specs=[kept((D, TOKENS)), kept((TOKENS, D)), columns_tile(), columns_tile(), deep_tile(0), ANY, VMEM],
        out_specs=[VMEM] * 5 + [ANY] * 2,
        scratch_shapes=[*STAGES, pltpu.VMEM((TOKENS, TILE), BF16), pltpu.VMEM((TOKENS, TILE), BF16), *sums.scratch_shapes, *NORM],
        compiler_params=pltpu.CompilerParams(collective_id=number, has_side_effects=True, vmem_limit_bytes=VMEM_LIMIT),
        name="first_sums",
    )(a1t, dh, gate, up, w_down, down.reshape(4, 4, 176, D), others)
    return d, g, u, total


AROUND = (1, -1, 2)
SCALAR = (8, 128)
NORM = [
    pltpu.VMEM((3, 3, *SCALAR), F32),
    pltpu.VMEM((4, *SCALAR), F32),
    pltpu.SemaphoreType.DMA((3, 3)),
    pltpu.SemaphoreType.DMA((3, 3)),
]


def norm(own, out, got, held, send, recv):
    held[0] = jnp.full(SCALAR, own, F32)
    for axis in AXES:
        copies = [
            pltpu.make_async_remote_copy(
                src_ref=held.at[axis],
                dst_ref=got.at[axis, n],
                send_sem=send.at[axis, n],
                recv_sem=recv.at[axis, n],
                device_id=at(axis, by),
                device_id_type=MESH,
            )
            for n, by in enumerate(AROUND)
        ]
        for copy in copies:
            copy.start()
        for copy in copies:
            copy.wait_recv()
        held[axis + 1] = (held[axis] + got[axis, 2]) + (got[axis, 0] + got[axis, 1])
        for copy in copies:
            copy.wait_send()
    out[...] = held[3]


class GatherJob:
    def __init__(self, form, colour, remote, local):
        self.form = form
        self.colour, self.first, self.width = colour
        self.axes = [(self.colour + n) % 3 for n in AXES]
        self.numbers = [[remote.new() for _ in range(4)] for _ in AXES]
        self.local_number = local.new()

    def bind(self, own, out, send, recv, local):
        self.own, self.out, self.send, self.recv, self.local = own, out, send, recv, local

    def held(self, n, by, layer=None):
        index = []
        for axis in AXES:
            if axis in self.axes[:n]:
                index.append(slice(None))
                continue
            k = place(axis, by if axis == self.axes[n] else 0)
            window = WINDOW[self.form]
            index.append(pl.ds(pl.multiple_of(k * window, 8), window) if axis == 2 else pl.ds(k, 1))
        layers = slice(None) if layer is None else pl.ds(layer, 1)
        return self.out.at[(layers, *index, pl.ds(self.first, self.width))]

    def copy(self, n, which):
        axis, number = self.axes[n], self.numbers[n][which]
        if which < 2:
            by = (1, -1)[which]
            source = self.own.at[:, :, :, :, pl.ds(self.first, self.width)] if n == 0 else self.held(n, 0)
            target = self.held(n, 0)
        else:
            by = (1, -1)[which - 2]
            source = target = self.held(n, -by, which - 2)
        return pltpu.make_async_remote_copy(
            src_ref=source,
            dst_ref=target,
            send_sem=self.send.at[number],
            recv_sem=self.recv.at[number],
            device_id=at(axis, by),
            device_id_type=MESH,
        )

    def keep(self):
        return pltpu.make_async_copy(
            self.own.at[:, :, :, :, pl.ds(self.first, self.width)], self.held(0, 0), self.local.at[self.local_number]
        )

    def actions(self):
        for n in AXES:

            def begin(n=n):
                if n == 0:
                    self.keep().start()
                else:
                    self.copy(n - 1, 2).wait_recv()
                    self.copy(n - 1, 3).wait_recv()
                if n == 1:
                    self.keep().wait()
                self.copy(n, 0).start()
                self.copy(n, 1).start()

            def forward(n=n):
                self.copy(n, 0).wait_recv()
                self.copy(n, 2).start()
                self.copy(n, 1).wait_recv()
                self.copy(n, 3).start()

            yield begin
            yield forward

        def last():
            self.copy(2, 2).wait_recv()
            self.copy(2, 3).wait_recv()
            for n in AXES:
                for which in range(4):
                    self.copy(n, which).wait_send()

        yield last


def gather_kernel(forms, number):
    remote, local = Copies(), Copies()
    jobs = [[GatherJob(form, colour, remote, local) for colour in COLOURS[form]] for form in forms]

    def kernel(*refs):
        owns, outs = refs[: len(forms)], refs[len(forms) : 2 * len(forms)]
        send, recv, loc = refs[2 * len(forms) :]
        greet(NEXT)
        order = []
        for m, of_matrix in enumerate(jobs):
            for j, job in enumerate(of_matrix):
                job.bind(owns[m], outs[m], send, recv, loc)
                for stage, action in enumerate(job.actions()):
                    order.append((stage, m, j, action))
        for *_, action in sorted(order, key=lambda o: o[:3]):
            action()

    def call(*owns):
        return pl.pallas_call(
            kernel,
            out_shape=[pltpu.VMEM((2, 4, 4, 4 * WINDOW[f], COLUMNS[f]), BF16) for f in forms],
            in_specs=[VMEM] * len(forms),
            out_specs=[VMEM] * len(forms),
            scratch_shapes=[
                pltpu.SemaphoreType.DMA((remote.count,)),
                pltpu.SemaphoreType.DMA((remote.count,)),
                pltpu.SemaphoreType.DMA((local.count,)),
            ],
            compiler_params=pltpu.CompilerParams(collective_id=number, has_side_effects=True, vmem_limit_bytes=SMALL_LIMIT),
            name="gather",
        )(*(o.reshape(2, 1, 1, WINDOW[f], COLUMNS[f]) for o, f in zip(owns, forms, strict=True)))

    return call


def settle(gate, up, down):
    def kernel(gate, up, down, gate_out, up_out, down_out, wide, close, sem, close_sem):
        copies = [pltpu.make_async_copy(gate, gate_out, sem.at[0]), pltpu.make_async_copy(up, up_out, sem.at[1])]
        for copy in copies:
            copy.start()

        def put(t):
            return pltpu.make_async_copy(
                close.at[lax.rem(t, 2)], down_out.at[lax.div(t, 16), lax.rem(t, 16)], close_sem.at[lax.rem(t, 2)]
            )

        def step(t, _):
            @pl.when(t >= 2)
            def _():
                put(t - 2).wait()

            for z in range(4):
                block = down[lax.div(t, 16), lax.rem(t, 16), pl.ds(48 * z, 48), :]
                wide[pl.ds(44 * z, 48), :] = block.astype(F32)
            close[lax.rem(t, 2)] = wide[pl.ds(0, 176), :].astype(BF16)
            put(t).start()
            return 0

        lax.fori_loop(0, 32, step, 0)
        put(30).wait()
        put(31).wait()
        for copy in copies:
            copy.wait()

    return pl.pallas_call(
        kernel,
        out_shape=[jax.ShapeDtypeStruct(gate.shape, BF16)] * 2 + [jax.ShapeDtypeStruct((2, 16, 176, D), BF16)],
        in_specs=[VMEM] * 3,
        out_specs=[ANY] * 3,
        scratch_shapes=[
            pltpu.VMEM((184, D), F32),
            pltpu.VMEM((2, 176, D), BF16),
            PAIR,
            PAIR,
        ],
        compiler_params=pltpu.CompilerParams(vmem_limit_bytes=SMALL_LIMIT),
        name="settle",
    )(gate, up, down.reshape(2, 16, 192, D))


def through_norm(dy, da, h):
    wide, da = h.astype(F32), da.astype(F32)
    scale = lax.rsqrt(jnp.mean(wide**2, -1, keepdims=True) + 1e-6)
    along = jnp.mean(da * wide, -1, keepdims=True) * scale**3
    return dy + (da * scale - wide * along).astype(BF16)


def adamw(w, m, v, g):
    m = 0.9 * m + 0.1 * g
    v = 0.95 * v + 0.05 * g * g
    step = m * lax.rsqrt(v + 1e-8) + 0.1 * w
    return (w - 0.02 * step).astype(BF16), m, v


def solution(mesh):
    def step(x, dy, *arrays):
        weights, m, v = (arrays[i : i + 3] for i in (0, 3, 6))
        x, dy = x[0], dy[0]
        w_gate, w_up, w_down = weights
        z = lax.rem(lax.axis_index("dp"), 4)
        gate1, up1, s1, a1t, h1, a2, a2t = first_layer(x, w_gate, w_up, w_down)
        dg, du, down2 = second_layer(a2, dy, w_gate, w_up, w_down)
        down_2, gate_2, up_2, squares_2, da2 = second_sums(a2t, dg, du, w_gate, w_up, down2, 0)
        down1, dh = down_term(s1, dy, da2, h1)
        down_1, gate_1, up_1, total = first_sums(a1t, dh, gate1, up1, w_down, down1, squares_2, 1)
        gate, up = (gate_1, gate_2), (up_1, up_2)
        down = [lax.dynamic_slice_in_dim(d, 4 * lax.rem(z, 2), 44, 0) for d in (down_1, down_2)]
        gradients = [jnp.stack(g).astype(F32) for g in (gate, up, down)]
        factor = jnp.minimum(1.0, 0.5 * lax.rsqrt(total[0, 0] / (6 * D * FF) + 1e-30))
        new = []
        for w, m_, v_, g in zip(weights, m, v, gradients, strict=True):
            rows = g.shape[1]
            own = lax.dynamic_slice_in_dim(w, lax.axis_index("dp") * rows, rows, 1)
            new.append(adamw(own.astype(F32), m_, v_, g * factor))
        own = [one[0] for one in new]
        own[2] = jnp.pad(own[2], ((0, 0), (0, 4), (0, 0)))
        gate, up, down = settle(*gather_kernel((WIDE, WIDE, DEEP), 2)(*own))
        return (
            gate.reshape(2, D, FF),
            up.reshape(2, D, FF),
            down.reshape(2, FF, D),
            *(one[1] for one in new),
            *(one[2] for one in new),
        )

    whole, rows = P(None, None, None), P(None, "dp", None)
    tokens, out, out_rows = P(("rep", "dp"), None, None), P("rep", None, None), P("rep", "dp", None)
    return jax.shard_map(
        step,
        mesh=mesh,
        in_specs=(tokens, tokens, *[whole] * 3, *[rows] * 6),
        out_specs=(*[out] * 3, *[out_rows] * 6),
        check_vma=False,
    )
```

```python
import functools

import jax
import jax.numpy as jnp
from jax import lax
from jax.experimental import pallas as pl
from jax.experimental.pallas import tpu as pltpu
from jax.sharding import PartitionSpec as P

NAMES = ("w_gate", "w_up", "w_down")
AXES = range(3)
PAIR = pltpu.SemaphoreType.DMA((2,))
BF16, F32 = jnp.bfloat16, jnp.float32
MESH = pl.DeviceIdType.MESH
VMEM_LIMIT, SMALL_LIMIT = 63 << 20, 8 << 20
TOKENS, D, FF = 2048, 1024, 2816
WIDE, DEEP = "wide", "deep"
ROWS = {WIDE: 64, DEEP: 176}
WINDOW = {WIDE: 16, DEEP: 48}
COLUMNS = {WIDE: FF, DEEP: D}
TILE = 256
TILES = FF // TILE


def laid(widths, kind):
    return tuple((*kind(n), sum(widths[:n]), width) for n, width in enumerate(widths))


WIDTHS = [2 * TILE] * 3 + [TILE] * 4 + [TILE // 2] * 2
READY = (2, 4, 6, 7, 8, 9, 10, 11, 11)
GATE = laid(WIDTHS, lambda n: (n % 3, 1 - 2 * (n // 3 % 2)))
UP = laid(WIDTHS, lambda n: ((n + 1) % 3, 2 * (n // 3 % 2) - 1))
DOWN = laid((256, 128, 128, 128, 128, 256), lambda n: (n // 2, 1 - 2 * (n % 2)))
COLOURS = {
    WIDE: laid((896, 896, 1024), lambda n: (n,)),
    DEEP: laid((384, 384, 256), lambda n: (n,)),
}
SECOND_DOWN, SECOND_WIDE, SECOND_LATE = (0, 4, 8, 15, 17, 19, 27), (0, 3, 6, 10, 12, 13, 21), (0, 4, 6, 7, 8, 10, 14)
FIRST_DOWN, FIRST_WIDE = (0, 5, 9, 19, 21, 42, 70), (0, 3, 8, 13, 28, 50, 69)


def coordinates():
    i = lax.axis_index("dp")
    return [lax.div(i, 16), lax.rem(lax.div(i, 4), 4), lax.rem(i, 4)]


def at(axis, by):
    c = coordinates()
    c[axis] = lax.rem(c[axis] + by + 4, 4)
    return {"dp": c[0] * 16 + c[1] * 4 + c[2]}


def place(axis, by):
    return lax.rem(coordinates()[axis] + by + 4, 4)


def greet(offsets):
    barrier = pltpu.get_barrier_semaphore()
    for axis, by in offsets:
        pl.semaphore_signal(barrier, inc=1, device_id=at(axis, by), device_id_type=MESH)
    pl.semaphore_wait(barrier, len(offsets))


NEXT = tuple((axis, by) for axis in AXES for by in (1, -1))


def first_row(form, z):
    if form == WIDE:
        return pl.multiple_of(z * 16, 8)
    return pl.multiple_of(lax.div(z, 2) * 88 + lax.rem(z, 2) * 40, 8)


def part(form, axis, k):
    index = [slice(None)] * 3
    index[axis] = pl.ds(first_row(form, k), WINDOW[form]) if axis == 2 else pl.ds(k, 1)
    return tuple(index)


def extent(form, done):
    return (1 if 0 in done else 4, 1 if 1 in done else 4, WINDOW[form] if 2 in done else ROWS[form])


class Scratch:
    def __init__(self):
        self.shapes = []

    def new(self, shape, dtype):
        self.shapes.append(pltpu.VMEM(shape, dtype))
        return len(self.shapes) - 1


class Copies:
    def __init__(self):
        self.count = 0

    def new(self):
        self.count += 1
        return self.count - 1


def each(shape, body):
    def step(t, _):
        body(lax.div(t, shape[1]), lax.rem(t, shape[1]))
        return 0

    lax.fori_loop(0, shape[0] * shape[1], step, 0)


class SumJob:
    def __init__(self, form, job, scratch, remote, local):
        self.form = form
        self.colour, self.d, self.first, self.width = job
        self.axes = [(self.colour + n) % 3 for n in AXES]
        done = []
        self.phases = []
        for n, axis in enumerate(self.axes):
            done.append(axis)
            shape = (*extent(form, done), self.width)
            names = {}
            for name in ("r1", "ro", "rm", "sm"):
                names[name] = scratch.new(shape, BF16)
            if n == 0:
                names["l1"], names["l0"] = local.new(), local.new()
            else:
                names["s1"] = scratch.new(shape, BF16)
                names["so"] = scratch.new(shape, BF16)
            if n < 2:
                names["acc"] = scratch.new(shape, F32)
            for name in ("c1", "co", "cm"):
                names[name] = remote.new()
            self.phases.append((axis, shape, names))

    def bind(self, source, out, squares, refs, send, recv, local):
        self.source, self.out, self.squares = source, out, squares
        self.refs, self.send, self.recv, self.local = refs, send, recv, local

    def buf(self, n, name):
        return self.refs[self.phases[n][2][name]]

    def copy(self, n, which):
        axis, _, names = self.phases[n]
        d = self.d
        target, by = {"c1": ("r1", d), "co": ("ro", -d), "cm": ("rm", d)}[which]
        if which == "cm":
            source = self.buf(n, "sm")
        elif n == 0:
            k = place(axis, 2 if which == "c1" else -d)
            source = self.source.at[(*part(self.form, axis, k), pl.ds(self.first, self.width))]
        else:
            source = self.buf(n, "s1" if which == "c1" else "so")
        number = names[which]
        return pltpu.make_async_remote_copy(
            src_ref=source,
            dst_ref=self.buf(n, target),
            send_sem=self.send.at[number],
            recv_sem=self.recv.at[number],
            device_id=at(axis, by),
            device_id_type=MESH,
        )

    def load(self, which):
        axis, _, names = self.phases[0]
        k = place(axis, self.d if which == "l1" else 0)
        return pltpu.make_async_copy(
            self.source.at[(*part(self.form, axis, k), pl.ds(self.first, self.width))],
            self.buf(0, "sm" if which == "l1" else "r1"),
            self.local.at[names[which]],
        )

    def rows(self, n, k):
        axis = self.phases[n][0]
        acc = self.buf(n - 1, "acc")

        def read(i, j):
            if axis == 0:
                return acc[k, j]
            if axis == 1:
                return acc[i, k]
            return acc[i, j, pl.ds(first_row(self.form, k), WINDOW[self.form]), :]

        return read

    def begin(self, n):
        axis, shape, _ = self.phases[n]
        if n == 0:
            self.copy(0, "c1").start()
            self.load("l1").start()
            self.copy(0, "co").start()
            return
        for name, by, copy in (("s1", 2, "c1"), ("so", -self.d, "co")):
            read, buf = self.rows(n, place(axis, by)), self.buf(n, name)

            def body(i, j):
                buf[i, j] = read(i, j).astype(BF16)

            each(shape, body)
            self.copy(n, copy).start()

    def middle(self, n):
        axis, shape, _ = self.phases[n]
        r1, sm = self.buf(n, "r1"), self.buf(n, "sm")
        if n == 0:
            self.load("l1").wait()
            read = lambda i, j: sm[i, j].astype(F32)
        else:
            read = self.rows(n, place(axis, self.d))
        self.copy(n, "c1").wait_recv()

        def body(i, j):
            sm[i, j] = (read(i, j) + r1[i, j].astype(F32)).astype(BF16)

        each(shape, body)
        self.copy(n, "cm").start()
        if n == 0:
            self.load("l0").start()

    def end(self, n):
        axis, shape, _ = self.phases[n]
        rm, ro = self.buf(n, "rm"), self.buf(n, "ro")
        if n == 0:
            self.load("l0").wait()
            own = self.buf(0, "r1")
            read = lambda i, j: own[i, j].astype(F32)
        else:
            read = self.rows(n, place(axis, 0))
        self.copy(n, "co").wait_recv()
        self.copy(n, "cm").wait_recv()

        def total(i, j):
            return read(i, j) + rm[i, j].astype(F32) + ro[i, j].astype(F32)

        if n < 2:
            acc = self.buf(n, "acc")

            def body(i, j):
                acc[i, j] = total(i, j)

            each(shape, body)
            return
        g = total(0, 0).astype(BF16)
        self.out[:, pl.ds(self.first, self.width)] = g
        square = g.astype(F32)
        square = square * square
        if self.form == DEEP:
            row = lax.broadcasted_iota(jnp.int32, square.shape, 0) - 4 * lax.rem(coordinates()[2], 2)
            square = jnp.where((row >= 0) & (row < 44), square, 0.0)
        square = jnp.sum(square, axis=0, keepdims=True)
        for t in range(self.width // 128):
            self.squares[...] += square[:, 128 * t : 128 * (t + 1)]

    def sent(self):
        for n in AXES:
            for which in ("c1", "co", "cm"):
                self.copy(n, which).wait_send()

    def actions(self):
        yield lambda: self.begin(0)
        yield lambda: self.middle(0)
        for n in (1, 2):

            def turn(n=n):
                self.end(n - 1)
                self.begin(n)

            yield turn
            yield lambda n=n: self.middle(n)

        def last():
            self.end(2)
            self.sent()

        yield last


class Sums:
    def __init__(self, matrices):
        self.scratch, self.remote, self.local = Scratch(), Copies(), Copies()
        self.forms = [form for form, *_ in matrices]
        self.jobs = []
        for m, (form, jobs, begins, later) in enumerate(matrices):
            for job, begin in zip(jobs, begins, strict=True):
                self.jobs.append((m, SumJob(form, job, self.scratch, self.remote, self.local), [begin + n for n in later(begin)]))
        self.out_shape = [jax.ShapeDtypeStruct((WINDOW[f], COLUMNS[f]), BF16) for f in self.forms]
        self.out_shape.append(jax.ShapeDtypeStruct((1, 128), F32))
        self.scratch_shapes = [
            *self.scratch.shapes,
            pltpu.SemaphoreType.DMA((self.remote.count,)),
            pltpu.SemaphoreType.DMA((self.remote.count,)),
            pltpu.SemaphoreType.DMA((self.local.count,)),
        ]

    def run(self, step, steps, parts, sources, outs, refs):
        *outs, squares = outs
        *refs, send, recv, local = refs
        due, end = {}, steps * parts
        for j, (m, job, times) in enumerate(self.jobs):
            job.bind(sources[m], outs[m], squares, refs, send, recv, local)
            for stage, (time, action) in enumerate(zip(times, job.actions(), strict=True)):
                due.setdefault(min(time, end), []).append((time, stage, j, action))

        def now(time):
            for *_, action in sorted(due.get(time, ()), key=lambda o: o[:3]):
                action()

        def reach(part):
            for time in range(part, end, parts):
                if time in due:
                    pl.when(step == time // parts)(functools.partial(now, time))

        def rest():
            pl.when(step == steps - 1)(functools.partial(now, end))

        def enter(offsets):
            @pl.when(step == 0)
            def _():
                greet(offsets)
                squares[...] = jnp.zeros_like(squares)

        return enter, reach, rest


def dot(a, b, dims=((1,), (0,))):
    return lax.dot_general(a, b, (dims, ((), ())), preferred_element_type=F32)


NT, TN = ((1,), (1,)), ((0,), (0,))
BLOCK, PART = 1024, 256


def blocks(n, size, body):
    lax.fori_loop(0, n // size, lambda t, _: (body(pl.ds(pl.multiple_of(t * size, size), size)), 0)[1], 0)


def kept(shape):
    return pl.BlockSpec(shape, lambda i: (0,) * len(shape), pipeline_mode=pl.Buffered(1))


def wide_tile(number, turn=lambda i: i):
    return pl.BlockSpec((None, D, TILE), lambda i: (number, 0, turn(i)))


def deep_tile(number):
    return pl.BlockSpec((None, TILE, D), lambda i: (number, i, 0))


def columns_tile(turn=lambda i: i):
    return pl.BlockSpec((TOKENS, TILE), lambda i: (0, turn(i)))


ANY = pl.BlockSpec(memory_space=pl.ANY)
VMEM = pl.BlockSpec(memory_space=pltpu.VMEM)


def normed_block(wide):
    return (wide * lax.rsqrt(jnp.mean(wide * wide, -1, keepdims=True) + 1e-6)).astype(BF16)


def first_layer(x, w_gate, w_up, w_down):
    def kernel(x, wg, wu, wd, gate, up, s, a1t, h1, a2, a2t, a_s, h_s, t_s, acc, sem):
        i = pl.program_id(0)

        def put(n, source, target):
            return pltpu.make_async_copy(source, target, sem.at[n])

        @pl.when(i == 0)
        def _():
            def body(rows):
                a = normed_block(x[rows, :].astype(F32))
                a_s[rows, :] = a
                t_s[:, rows] = a.T
                acc[rows, :] = jnp.zeros((TILE, D), F32)

            blocks(TOKENS, TILE, body)
            put(0, t_s, a1t).start()

        def body(rows):
            a = a_s[rows, :]
            g = dot(a, wg[...])
            u = dot(a, wu[...])
            gate[rows, :] = g
            up[rows, :] = u
            p = (g * lax.logistic(g) * u).astype(BF16)
            s[rows, :] = p
            acc[rows, :] += dot(p, wd[...])

        blocks(TOKENS, BLOCK, body)

        @pl.when(i == TILES - 1)
        def _():
            put(0, t_s, a1t).wait()

            def body(rows):
                h = x[rows, :] + acc[rows, :].astype(BF16)
                h_s[rows, :] = h
                a = normed_block(h.astype(F32))
                a_s[rows, :] = a
                t_s[:, rows] = a.T

            blocks(TOKENS, TILE, body)
            copies = [put(0, t_s, a2t), put(1, h_s, h1), put(2, a_s, a2)]
            for copy in copies:
                copy.start()
            for copy in copies:
                copy.wait()

    tokens, turned = jax.ShapeDtypeStruct((TOKENS, D), BF16), jax.ShapeDtypeStruct((D, TOKENS), BF16)
    hidden = (TOKENS, FF)
    return pl.pallas_call(
        kernel,
        grid=(TILES,),
        out_shape=[
            jax.ShapeDtypeStruct(hidden, F32),
            jax.ShapeDtypeStruct(hidden, F32),
            jax.ShapeDtypeStruct(hidden, BF16),
            turned,
            tokens,
            tokens,
            turned,
        ],
        in_specs=[kept((TOKENS, D)), wide_tile(0), wide_tile(0), deep_tile(0)],
        out_specs=[columns_tile()] * 3 + [ANY] * 4,
        scratch_shapes=[
            pltpu.VMEM((TOKENS, D), BF16),
            pltpu.VMEM((TOKENS, D), BF16),
            pltpu.VMEM((D, TOKENS), BF16),
            pltpu.VMEM((TOKENS, D), F32),
            pltpu.SemaphoreType.DMA((3,)),
        ],
        compiler_params=pltpu.CompilerParams(vmem_limit_bytes=VMEM_LIMIT),
        name="first_layer",
    )(x, w_gate, w_up, w_down)


def through_product(ds, g, u):
    sig = lax.logistic(g)
    silu = g * sig
    return (ds * u * (sig + silu * (1.0 - sig))).astype(BF16), (ds * silu).astype(BF16)


def second_layer(a2, dy, w_gate, w_up, w_down):
    def kernel(a2, dy, wg, wu, wd, dg, du, dwd, s):
        def body(rows):
            a = a2[rows, :]
            g = dot(a, wg[...])
            u = dot(a, wu[...])
            ds = dot(dy[rows, :], wd[...], NT).astype(BF16).astype(F32)
            s[rows, :] = (g * lax.logistic(g) * u).astype(BF16)
            dg[rows, :], du[rows, :] = through_product(ds, g, u)

        blocks(TOKENS, BLOCK, body)
        dwd[...] = dot(s[...], dy[...], TN).astype(BF16)

    return pl.pallas_call(
        kernel,
        grid=(TILES,),
        out_shape=[jax.ShapeDtypeStruct((TOKENS, FF), BF16)] * 2 + [jax.ShapeDtypeStruct((FF, D), BF16)],
        in_specs=[kept((TOKENS, D))] * 2 + [wide_tile(1), wide_tile(1), deep_tile(1)],
        out_specs=[columns_tile()] * 2 + [pl.BlockSpec((TILE, D), lambda i: (i, 0))],
        scratch_shapes=[pltpu.VMEM((TOKENS, TILE), BF16)],
        compiler_params=pltpu.CompilerParams(vmem_limit_bytes=VMEM_LIMIT),
        name="second_layer",
    )(a2, dy, w_gate, w_up, w_down)


def down_term(s, dh):
    def kernel(s, dh, out):
        out[...] = dot(s[...], dh[...], TN).astype(BF16)

    return pl.pallas_call(
        kernel,
        grid=(TILES,),
        out_shape=jax.ShapeDtypeStruct((FF, D), BF16),
        in_specs=[columns_tile(), kept((TOKENS, D))],
        out_specs=pl.BlockSpec((TILE, D), lambda i: (i, 0)),
        compiler_params=pltpu.CompilerParams(vmem_limit_bytes=VMEM_LIMIT),
        name="down_term",
    )(s, dh)


def store_terms(at, dg, du, stage_g, stage_u):
    for stage, cotangent in ((stage_g, dg), (stage_u, du)):
        stage[...] = dot(at[...], cotangent[...]).astype(BF16).reshape(stage.shape)


class Terms:
    def __init__(self, stages, terms, sem):
        self.stages, self.terms, self.sem = stages, terms, sem

    def copies(self, tile):
        columns = pl.ds(pl.multiple_of(tile * TILE, TILE), TILE)
        return [
            pltpu.make_async_copy(stage, term.at[:, :, :, columns], self.sem.at[n])
            for n, (stage, term) in enumerate(zip(self.stages, self.terms, strict=True))
        ]

    def start(self, tile):
        for copy in self.copies(tile):
            copy.start()

    def wait(self, tile):
        for copy in self.copies(tile):
            copy.wait()


TERM = jax.ShapeDtypeStruct((4, 4, 64, FF), BF16)
STAGES = [pltpu.VMEM((4, 4, 64, TILE), BF16)] * 2 + [PAIR]


def second_sums(a2t, dg, du, w_gate, w_up, down, dy, h1, number):
    steps = 2 * TILES
    later = lambda begin: SECOND_LATE if begin >= 9 else SECOND_WIDE
    sums = Sums(
        (
            (DEEP, DOWN, (0,) * 6, lambda begin: SECOND_DOWN),
            (WIDE, GATE, READY, later),
            (WIDE, UP, READY, later),
        )
    )

    def kernel(a2t, dg, du, wg, wu, down, dy, h1, *refs):
        outs, refs = refs[:4], refs[4:]
        dh, term_g, term_u, stage_g, stage_u, term_sem, acc, half, half_sem, taken, taken_sem, *refs = refs
        i = pl.program_id(0)
        terms = Terms((stage_g, stage_u), (term_g, term_u), term_sem)
        enter, reach, rest = sums.run(i, steps, 1, (down, term_g, term_u), outs, refs)
        enter(NEXT)

        @pl.when((i > 0) & (i <= TILES))
        def _():
            terms.wait(i - 1)

        reach(0)

        @pl.when(i < TILES)
        def _():
            store_terms(a2t, dg, du, stage_g, stage_u)
            terms.start(i)

        @pl.when(i == TILES)
        def _():
            blocks(TOKENS, TILE, lambda rows: acc.__setitem__((rows, slice(None)), jnp.zeros((TILE, D), F32)))

        @pl.when(i >= TILES)
        def _():
            def body(rows):
                acc[rows, :] += dot(dg[rows, :], wg[...], NT) + dot(du[rows, :], wu[...], NT)

            blocks(TOKENS, BLOCK, body)

        def take(n):
            rows = pl.ds(PART * n, PART)
            return [
                pltpu.make_async_copy(source.at[rows, :], taken.at[n % 2, which], taken_sem.at[n % 2, which])
                for which, source in enumerate((dy, h1))
            ]

        def give(n):
            return pltpu.make_async_copy(half.at[n % 2], dh.at[pl.ds(PART * n, PART), :], half_sem.at[n % 2])

        @pl.when(i == steps - 1)
        def _():
            parts = TOKENS // PART
            for copy in take(0):
                copy.start()
            for n in range(parts):
                if n + 1 < parts:
                    for copy in take(n + 1):
                        copy.start()
                for copy in take(n):
                    copy.wait()
                if n >= 2:
                    give(n - 2).wait()

                def body(rows, n=n):
                    da = acc[pl.ds(pl.multiple_of(PART * n + rows.start, 8), rows.size), :].astype(BF16)
                    half[n % 2, rows, :] = through_norm(taken[n % 2, 0, rows, :], da, taken[n % 2, 1, rows, :])

                blocks(PART, PART // 2, body)
                give(n).start()
            give(parts - 2).wait()
            give(parts - 1).wait()

        rest()

    turn = lambda i: lax.rem(i, TILES)
    late = lambda i: jnp.maximum(i - TILES, 0)
    d, g, u, squares, dh, *_ = pl.pallas_call(
        kernel,
        grid=(steps,),
        out_shape=[*sums.out_shape, jax.ShapeDtypeStruct((TOKENS, D), BF16), TERM, TERM],
        in_specs=[kept((D, TOKENS)), columns_tile(turn), columns_tile(turn), wide_tile(1, late), wide_tile(1, late), ANY, ANY, ANY],
        out_specs=[VMEM] * 4 + [ANY] * 3,
        scratch_shapes=[
            *STAGES,
            pltpu.VMEM((TOKENS, D), F32),
            pltpu.VMEM((2, PART, D), BF16),
            PAIR,
            pltpu.VMEM((2, 2, PART, D), BF16),
            pltpu.SemaphoreType.DMA((2, 2)),
            *sums.scratch_shapes,
        ],
        compiler_params=pltpu.CompilerParams(collective_id=number, has_side_effects=True, vmem_limit_bytes=VMEM_LIMIT),
        name="second_sums",
    )(a2t, dg, du, w_gate, w_up, down.reshape(4, 4, 176, D), dy, h1)
    return d, g, u, squares, dh


def first_sums(a1t, dh, gate, up, w_down, down, others, number):
    steps = TILES
    sums = Sums(
        (
            (DEEP, DOWN, (0,) * 6, lambda begin: FIRST_DOWN),
            (WIDE, GATE, [2 * n for n in READY], lambda begin: FIRST_WIDE),
            (WIDE, UP, [2 * n for n in READY], lambda begin: FIRST_WIDE),
        )
    )

    def kernel(a1t, dh, gate, up, wd, down, others, *refs):
        outs, refs = refs[:4], refs[4:]
        total, term_g, term_u, stage_g, stage_u, term_sem, dg, du, *refs = refs
        *refs, got, held, norm_send, norm_recv = refs
        i = pl.program_id(0)
        terms = Terms((stage_g, stage_u), (term_g, term_u), term_sem)
        enter, reach, rest = sums.run(i, steps, 2, (down, term_g, term_u), outs, refs)
        enter([(axis, by) for axis in AXES for by in AROUND])

        @pl.when(i > 0)
        def _():
            terms.wait(i - 1)

        reach(0)

        def body(rows):
            ds = dot(dh[rows, :], wd[...], NT).astype(BF16).astype(F32)
            dg[rows, :], du[rows, :] = through_product(ds, gate[rows, :], up[rows, :])

        blocks(TOKENS, BLOCK, body)
        reach(1)
        store_terms(a1t, dg, du, stage_g, stage_u)
        terms.start(i)

        @pl.when(i == steps - 1)
        def _():
            terms.wait(i)

        rest()

        @pl.when(i == steps - 1)
        def _():
            norm(jnp.sum(outs[3][...] + others[...]), total, got, held, norm_send, norm_recv)

    d, g, u, _, total, *_ = pl.pallas_call(
        kernel,
        grid=(steps,),
        out_shape=[*sums.out_shape, jax.ShapeDtypeStruct(SCALAR, F32), TERM, TERM],
        in_specs=[kept((D, TOKENS)), kept((TOKENS, D)), columns_tile(), columns_tile(), deep_tile(0), ANY, VMEM],
        out_specs=[VMEM] * 5 + [ANY] * 2,
        scratch_shapes=[*STAGES, pltpu.VMEM((TOKENS, TILE), BF16), pltpu.VMEM((TOKENS, TILE), BF16), *sums.scratch_shapes, *NORM],
        compiler_params=pltpu.CompilerParams(collective_id=number, has_side_effects=True, vmem_limit_bytes=VMEM_LIMIT),
        name="first_sums",
    )(a1t, dh, gate, up, w_down, down.reshape(4, 4, 176, D), others)
    return d, g, u, total


AROUND = (1, -1, 2)
SCALAR = (8, 128)
NORM = [
    pltpu.VMEM((3, 3, *SCALAR), F32),
    pltpu.VMEM((4, *SCALAR), F32),
    pltpu.SemaphoreType.DMA((3, 3)),
    pltpu.SemaphoreType.DMA((3, 3)),
]


def norm(own, out, got, held, send, recv):
    held[0] = jnp.full(SCALAR, own, F32)
    for axis in AXES:
        copies = [
            pltpu.make_async_remote_copy(
                src_ref=held.at[axis],
                dst_ref=got.at[axis, n],
                send_sem=send.at[axis, n],
                recv_sem=recv.at[axis, n],
                device_id=at(axis, by),
                device_id_type=MESH,
            )
            for n, by in enumerate(AROUND)
        ]
        for copy in copies:
            copy.start()
        for copy in copies:
            copy.wait_recv()
        held[axis + 1] = (held[axis] + got[axis, 2]) + (got[axis, 0] + got[axis, 1])
        for copy in copies:
            copy.wait_send()
    out[...] = held[3]


class GatherJob:
    def __init__(self, form, colour, remote, local):
        self.form = form
        self.colour, self.first, self.width = colour
        self.axes = [(self.colour + n) % 3 for n in AXES]
        self.numbers = [[remote.new() for _ in range(4)] for _ in AXES]
        self.local_number = local.new()

    def bind(self, own, out, send, recv, local):
        self.own, self.out, self.send, self.recv, self.local = own, out, send, recv, local

    def held(self, n, by, layer=None):
        index = []
        for axis in AXES:
            if axis in self.axes[:n]:
                index.append(slice(None))
                continue
            k = place(axis, by if axis == self.axes[n] else 0)
            window = WINDOW[self.form]
            index.append(pl.ds(pl.multiple_of(k * window, 8), window) if axis == 2 else pl.ds(k, 1))
        layers = slice(None) if layer is None else pl.ds(layer, 1)
        return self.out.at[(layers, *index, pl.ds(self.first, self.width))]

    def copy(self, n, which):
        axis, number = self.axes[n], self.numbers[n][which]
        if which < 2:
            by = (1, -1)[which]
            source = self.own.at[:, :, :, :, pl.ds(self.first, self.width)] if n == 0 else self.held(n, 0)
            target = self.held(n, 0)
        else:
            by = (1, -1)[which - 2]
            source = target = self.held(n, -by, which - 2)
        return pltpu.make_async_remote_copy(
            src_ref=source,
            dst_ref=target,
            send_sem=self.send.at[number],
            recv_sem=self.recv.at[number],
            device_id=at(axis, by),
            device_id_type=MESH,
        )

    def keep(self):
        return pltpu.make_async_copy(
            self.own.at[:, :, :, :, pl.ds(self.first, self.width)], self.held(0, 0), self.local.at[self.local_number]
        )

    def actions(self):
        for n in AXES:

            def begin(n=n):
                if n == 0:
                    self.keep().start()
                else:
                    self.copy(n - 1, 2).wait_recv()
                    self.copy(n - 1, 3).wait_recv()
                if n == 1:
                    self.keep().wait()
                self.copy(n, 0).start()
                self.copy(n, 1).start()

            def forward(n=n):
                self.copy(n, 0).wait_recv()
                self.copy(n, 2).start()
                self.copy(n, 1).wait_recv()
                self.copy(n, 3).start()

            yield begin
            yield forward

        def last():
            self.copy(2, 2).wait_recv()
            self.copy(2, 3).wait_recv()
            for n in AXES:
                for which in range(4):
                    self.copy(n, which).wait_send()

        yield last


def close_up(padded, closed, rows):
    def step(t, _):
        layer, pair = lax.div(t, 16), lax.rem(t, 16)
        for z in range(4):
            block = padded[layer, lax.div(pair, 4), lax.rem(pair, 4), pl.ds(48 * z, 48), :]
            rows[pl.ds(44 * z, 48), :] = block.astype(F32)
        closed[layer, pair] = rows[pl.ds(0, 176), :].astype(BF16)
        return 0

    lax.fori_loop(0, 32, step, 0)


def gather_kernel(forms, number):
    shapes = [(2, 4, 4, 4 * WINDOW[f], COLUMNS[f]) for f in forms]
    remote, local = Copies(), Copies()
    jobs = [[GatherJob(form, colour, remote, local) for colour in COLOURS[form]] for form in forms]

    def kernel(*refs):
        owns, (*outs, closed) = refs[: len(forms)], refs[len(forms) : 2 * len(forms)]
        padded, rows, send, recv, loc = refs[2 * len(forms) :]
        outs.append(padded)
        greet(NEXT)
        order = []
        for m, of_matrix in enumerate(jobs):
            for j, job in enumerate(of_matrix):
                job.bind(owns[m], outs[m], send, recv, loc)
                for stage, action in enumerate(job.actions()):
                    order.append((stage if forms[m] == DEEP else stage + 1.5, m, j, action))
        order.append((6.2, 0, 0, lambda: close_up(padded, closed, rows)))
        for *_, action in sorted(order, key=lambda o: o[:3]):
            action()

    def call(*owns):
        return pl.pallas_call(
            kernel,
            out_shape=[pltpu.VMEM(s, BF16) for s in (*shapes[:-1], (2, 16, 176, D))],
            in_specs=[VMEM] * len(forms),
            out_specs=[VMEM] * len(forms),
            scratch_shapes=[
                pltpu.VMEM(shapes[-1], BF16),
                pltpu.VMEM((184, D), F32),
                pltpu.SemaphoreType.DMA((remote.count,)),
                pltpu.SemaphoreType.DMA((remote.count,)),
                pltpu.SemaphoreType.DMA((local.count,)),
            ],
            compiler_params=pltpu.CompilerParams(collective_id=number, has_side_effects=True, vmem_limit_bytes=2 * SMALL_LIMIT),
            name="gather",
        )(*(o.reshape(2, 1, 1, WINDOW[f], COLUMNS[f]) for o, f in zip(owns, forms, strict=True)))

    return call


def settle(*weights):
    def kernel(*refs):
        sem = refs[-1]
        copies = [
            pltpu.make_async_copy(refs[n].at[layer], refs[3 + n].at[layer], sem.at[n, layer]) for n in AXES for layer in (0, 1)
        ]
        for copy in copies:
            copy.start()
        for copy in copies:
            copy.wait()

    return pl.pallas_call(
        kernel,
        out_shape=[jax.ShapeDtypeStruct(w.shape, BF16) for w in weights],
        in_specs=[VMEM] * 3,
        out_specs=[ANY] * 3,
        scratch_shapes=[pltpu.SemaphoreType.DMA((3, 2))],
        compiler_params=pltpu.CompilerParams(vmem_limit_bytes=SMALL_LIMIT),
        name="settle",
    )(*weights)


def through_norm(dy, da, h):
    wide, da = h.astype(F32), da.astype(F32)
    scale = lax.rsqrt(jnp.mean(wide**2, -1, keepdims=True) + 1e-6)
    along = jnp.mean(da * wide, -1, keepdims=True) * scale**3
    return dy + (da * scale - wide * along).astype(BF16)


def adamw(w, m, v, g):
    m = 0.9 * m + 0.1 * g
    v = 0.95 * v + 0.05 * g * g
    step = m * lax.rsqrt(v + 1e-8) + 0.1 * w
    return (w - 0.02 * step).astype(BF16), m, v


def solution(mesh):
    def step(x, dy, *arrays):
        weights, m, v = (arrays[i : i + 3] for i in (0, 3, 6))
        x, dy = x[0], dy[0]
        w_gate, w_up, w_down = weights
        z = lax.rem(lax.axis_index("dp"), 4)
        gate1, up1, s1, a1t, h1, a2, a2t = first_layer(x, w_gate, w_up, w_down)
        dg, du, down2 = second_layer(a2, dy, w_gate, w_up, w_down)
        down_2, gate_2, up_2, squares_2, dh = second_sums(a2t, dg, du, w_gate, w_up, down2, dy, h1, 0)
        down1 = down_term(s1, dh)
        down_1, gate_1, up_1, total = first_sums(a1t, dh, gate1, up1, w_down, down1, squares_2, 1)
        gate, up = (gate_1, gate_2), (up_1, up_2)
        down = [lax.dynamic_slice_in_dim(d, 4 * lax.rem(z, 2), 44, 0) for d in (down_1, down_2)]
        gradients = [jnp.stack(g).astype(F32) for g in (gate, up, down)]
        factor = jnp.minimum(1.0, 0.5 * lax.rsqrt(total[0, 0] / (6 * D * FF) + 1e-30))
        new = []
        for w, m_, v_, g in zip(weights, m, v, gradients, strict=True):
            rows = g.shape[1]
            own = lax.dynamic_slice_in_dim(w, lax.axis_index("dp") * rows, rows, 1)
            new.append(adamw(own.astype(F32), m_, v_, g * factor))
        own = [one[0] for one in new]
        own[2] = jnp.pad(own[2], ((0, 0), (0, 4), (0, 0)))
        gate, up, down = settle(*gather_kernel((WIDE, WIDE, DEEP), 2)(*own))
        return (
            gate.reshape(2, D, FF),
            up.reshape(2, D, FF),
            down.reshape(2, FF, D),
            *(one[1] for one in new),
            *(one[2] for one in new),
        )

    whole, rows = P(None, None, None), P(None, "dp", None)
    tokens, out, out_rows = P(("rep", "dp"), None, None), P("rep", None, None), P("rep", "dp", None)
    return jax.shard_map(
        step,
        mesh=mesh,
        in_specs=(tokens, tokens, *[whole] * 3, *[rows] * 6),
        out_specs=(*[out] * 3, *[out_rows] * 6),
        check_vma=False,
    )
```

```python
import functools

import jax
import jax.numpy as jnp
from jax import lax
from jax.experimental import pallas as pl
from jax.experimental.pallas import tpu as pltpu
from jax.sharding import PartitionSpec as P

NAMES = ("w_gate", "w_up", "w_down")
AXES = range(3)
PAIR = pltpu.SemaphoreType.DMA((2,))
BF16, F32 = jnp.bfloat16, jnp.float32
MESH = pl.DeviceIdType.MESH
VMEM_LIMIT, SMALL_LIMIT = 63 << 20, 8 << 20
TOKENS, D, FF = 2048, 1024, 2816
WIDE, DEEP = "wide", "deep"
ROWS = {WIDE: 64, DEEP: 176}
WINDOW = {WIDE: 16, DEEP: 48}
COLUMNS = {WIDE: FF, DEEP: D}
TILE = 256
TILES = FF // TILE


def laid(widths, kind):
    return tuple((*kind(n), sum(widths[:n]), width) for n, width in enumerate(widths))


WIDTHS = [2 * TILE] * 3 + [TILE] * 4 + [TILE // 2] * 2
READY = (2, 4, 6, 7, 8, 9, 10, 11, 11)
GATE = laid(WIDTHS, lambda n: (n % 3, 1 - 2 * (n // 3 % 2)))
UP = laid(WIDTHS, lambda n: ((n + 1) % 3, 2 * (n // 3 % 2) - 1))
DOWN = laid((256, 128, 128, 128, 128, 256), lambda n: (n // 2, 1 - 2 * (n % 2)))
COLOURS = {
    WIDE: laid((896, 896, 1024), lambda n: (n,)),
    DEEP: laid((384, 384, 256), lambda n: (n,)),
}
SECOND_DOWN, SECOND_WIDE, SECOND_LATE = (0, 4, 8, 15, 17, 19, 27), (0, 3, 6, 10, 12, 13, 21), (0, 4, 6, 7, 8, 10, 14)
FIRST_DOWN, FIRST_WIDE = (0, 4, 7, 9, 12, 23, 40), (0, 2, 5, 10, 17, 24, 37)


def coordinates():
    i = lax.axis_index("dp")
    return [lax.div(i, 16), lax.rem(lax.div(i, 4), 4), lax.rem(i, 4)]


def at(axis, by):
    c = coordinates()
    c[axis] = lax.rem(c[axis] + by + 4, 4)
    return {"dp": c[0] * 16 + c[1] * 4 + c[2]}


def place(axis, by):
    return lax.rem(coordinates()[axis] + by + 4, 4)


def greet(offsets):
    barrier = pltpu.get_barrier_semaphore()
    for axis, by in offsets:
        pl.semaphore_signal(barrier, inc=1, device_id=at(axis, by), device_id_type=MESH)
    pl.semaphore_wait(barrier, len(offsets))


NEXT = tuple((axis, by) for axis in AXES for by in (1, -1))


def first_row(form, z):
    if form == WIDE:
        return pl.multiple_of(z * 16, 8)
    return pl.multiple_of(lax.div(z, 2) * 88 + lax.rem(z, 2) * 40, 8)


def part(form, axis, k):
    index = [slice(None)] * 3
    index[axis] = pl.ds(first_row(form, k), WINDOW[form]) if axis == 2 else pl.ds(k, 1)
    return tuple(index)


def extent(form, done):
    return (1 if 0 in done else 4, 1 if 1 in done else 4, WINDOW[form] if 2 in done else ROWS[form])


class Scratch:
    def __init__(self):
        self.shapes = []

    def new(self, shape, dtype):
        self.shapes.append(pltpu.VMEM(shape, dtype))
        return len(self.shapes) - 1


class Copies:
    def __init__(self):
        self.count = 0

    def new(self):
        self.count += 1
        return self.count - 1


def each(shape, body):
    def step(t, _):
        body(lax.div(t, shape[1]), lax.rem(t, shape[1]))
        return 0

    lax.fori_loop(0, shape[0] * shape[1], step, 0)


class SumJob:
    def __init__(self, form, job, scratch, remote, local):
        self.form = form
        self.colour, self.d, self.first, self.width = job
        self.axes = [(self.colour + n) % 3 for n in AXES]
        done = []
        self.phases = []
        for n, axis in enumerate(self.axes):
            done.append(axis)
            shape = (*extent(form, done), self.width)
            names = {}
            for name in ("r1", "ro", "rm", "sm"):
                names[name] = scratch.new(shape, BF16)
            if n == 0:
                names["l1"], names["l0"] = local.new(), local.new()
            else:
                names["s1"] = scratch.new(shape, BF16)
                names["so"] = scratch.new(shape, BF16)
            if n < 2:
                names["acc"] = scratch.new(shape, F32)
            for name in ("c1", "co", "cm"):
                names[name] = remote.new()
            self.phases.append((axis, shape, names))

    def bind(self, source, out, squares, refs, send, recv, local):
        self.source, self.out, self.squares = source, out, squares
        self.refs, self.send, self.recv, self.local = refs, send, recv, local

    def buf(self, n, name):
        return self.refs[self.phases[n][2][name]]

    def copy(self, n, which):
        axis, _, names = self.phases[n]
        d = self.d
        target, by = {"c1": ("r1", d), "co": ("ro", -d), "cm": ("rm", d)}[which]
        if which == "cm":
            source = self.buf(n, "sm")
        elif n == 0:
            k = place(axis, 2 if which == "c1" else -d)
            source = self.source.at[(*part(self.form, axis, k), pl.ds(self.first, self.width))]
        else:
            source = self.buf(n, "s1" if which == "c1" else "so")
        number = names[which]
        return pltpu.make_async_remote_copy(
            src_ref=source,
            dst_ref=self.buf(n, target),
            send_sem=self.send.at[number],
            recv_sem=self.recv.at[number],
            device_id=at(axis, by),
            device_id_type=MESH,
        )

    def load(self, which):
        axis, _, names = self.phases[0]
        k = place(axis, self.d if which == "l1" else 0)
        return pltpu.make_async_copy(
            self.source.at[(*part(self.form, axis, k), pl.ds(self.first, self.width))],
            self.buf(0, "sm" if which == "l1" else "r1"),
            self.local.at[names[which]],
        )

    def rows(self, n, k):
        axis = self.phases[n][0]
        acc = self.buf(n - 1, "acc")

        def read(i, j):
            if axis == 0:
                return acc[k, j]
            if axis == 1:
                return acc[i, k]
            return acc[i, j, pl.ds(first_row(self.form, k), WINDOW[self.form]), :]

        return read

    def begin(self, n):
        axis, shape, _ = self.phases[n]
        if n == 0:
            self.copy(0, "c1").start()
            self.load("l1").start()
            self.copy(0, "co").start()
            return
        for name, by, copy in (("s1", 2, "c1"), ("so", -self.d, "co")):
            read, buf = self.rows(n, place(axis, by)), self.buf(n, name)

            def body(i, j):
                buf[i, j] = read(i, j).astype(BF16)

            each(shape, body)
            self.copy(n, copy).start()

    def middle(self, n):
        axis, shape, _ = self.phases[n]
        r1, sm = self.buf(n, "r1"), self.buf(n, "sm")
        if n == 0:
            self.load("l1").wait()
            read = lambda i, j: sm[i, j].astype(F32)
        else:
            read = self.rows(n, place(axis, self.d))
        self.copy(n, "c1").wait_recv()

        def body(i, j):
            sm[i, j] = (read(i, j) + r1[i, j].astype(F32)).astype(BF16)

        each(shape, body)
        self.copy(n, "cm").start()
        if n == 0:
            self.load("l0").start()

    def end(self, n):
        axis, shape, _ = self.phases[n]
        rm, ro = self.buf(n, "rm"), self.buf(n, "ro")
        if n == 0:
            self.load("l0").wait()
            own = self.buf(0, "r1")
            read = lambda i, j: own[i, j].astype(F32)
        else:
            read = self.rows(n, place(axis, 0))
        self.copy(n, "co").wait_recv()
        self.copy(n, "cm").wait_recv()

        def total(i, j):
            return read(i, j) + rm[i, j].astype(F32) + ro[i, j].astype(F32)

        if n < 2:
            acc = self.buf(n, "acc")

            def body(i, j):
                acc[i, j] = total(i, j)

            each(shape, body)
            return
        g = total(0, 0).astype(BF16)
        self.out[:, pl.ds(self.first, self.width)] = g
        square = g.astype(F32)
        square = square * square
        if self.form == DEEP:
            row = lax.broadcasted_iota(jnp.int32, square.shape, 0) - 4 * lax.rem(coordinates()[2], 2)
            square = jnp.where((row >= 0) & (row < 44), square, 0.0)
        square = jnp.sum(square, axis=0, keepdims=True)
        for t in range(self.width // 128):
            self.squares[...] += square[:, 128 * t : 128 * (t + 1)]

    def sent(self):
        for n in AXES:
            for which in ("c1", "co", "cm"):
                self.copy(n, which).wait_send()

    def actions(self):
        yield lambda: self.begin(0)
        yield lambda: self.middle(0)
        for n in (1, 2):

            def turn(n=n):
                self.end(n - 1)
                self.begin(n)

            yield turn
            yield lambda n=n: self.middle(n)

        def last():
            self.end(2)
            self.sent()

        yield last


class Sums:
    def __init__(self, matrices):
        self.scratch, self.remote, self.local = Scratch(), Copies(), Copies()
        self.forms = [form for form, *_ in matrices]
        self.jobs = []
        for m, (form, jobs, begins, later) in enumerate(matrices):
            for job, begin in zip(jobs, begins, strict=True):
                self.jobs.append((m, SumJob(form, job, self.scratch, self.remote, self.local), [begin + n for n in later(begin)]))
        self.out_shape = [jax.ShapeDtypeStruct((WINDOW[f], COLUMNS[f]), BF16) for f in self.forms]
        self.out_shape.append(jax.ShapeDtypeStruct((1, 128), F32))
        self.scratch_shapes = [
            *self.scratch.shapes,
            pltpu.SemaphoreType.DMA((self.remote.count,)),
            pltpu.SemaphoreType.DMA((self.remote.count,)),
            pltpu.SemaphoreType.DMA((self.local.count,)),
        ]

    def run(self, step, steps, parts, sources, outs, refs):
        *outs, squares = outs
        *refs, send, recv, local = refs
        due, end = {}, steps * parts
        for j, (m, job, times) in enumerate(self.jobs):
            job.bind(sources[m], outs[m], squares, refs, send, recv, local)
            for stage, (time, action) in enumerate(zip(times, job.actions(), strict=True)):
                due.setdefault(min(time, end), []).append((time, stage, j, action))

        def now(time):
            for *_, action in sorted(due.get(time, ()), key=lambda o: o[:3]):
                action()

        def reach(part):
            for time in range(part, end, parts):
                if time in due:
                    pl.when(step == time // parts)(functools.partial(now, time))

        def rest():
            pl.when(step == steps - 1)(functools.partial(now, end))

        def enter(offsets):
            @pl.when(step == 0)
            def _():
                greet(offsets)
                squares[...] = jnp.zeros_like(squares)

        return enter, reach, rest


def dot(a, b, dims=((1,), (0,))):
    return lax.dot_general(a, b, (dims, ((), ())), preferred_element_type=F32)


NT, TN = ((1,), (1,)), ((0,), (0,))
BLOCK, PART = 1024, 128


def blocks(n, size, body):
    lax.fori_loop(0, n // size, lambda t, _: (body(pl.ds(pl.multiple_of(t * size, size), size)), 0)[1], 0)


def kept(shape):
    return pl.BlockSpec(shape, lambda i: (0,) * len(shape), pipeline_mode=pl.Buffered(1))


def wide_tile(number, turn=lambda i: i):
    return pl.BlockSpec((None, D, TILE), lambda i: (number, 0, turn(i)))


def deep_tile(number):
    return pl.BlockSpec((None, TILE, D), lambda i: (number, i, 0))


def columns_tile(turn=lambda i: i):
    return pl.BlockSpec((TOKENS, TILE), lambda i: (0, turn(i)))


ANY = pl.BlockSpec(memory_space=pl.ANY)
VMEM = pl.BlockSpec(memory_space=pltpu.VMEM)


def normed_block(wide):
    return (wide * lax.rsqrt(jnp.mean(wide * wide, -1, keepdims=True) + 1e-6)).astype(BF16)


def first_layer(x, w_gate, w_up, w_down):
    def kernel(x, wg, wu, wd, gate, up, s, a1t, h1, a2, a2t, a_s, h_s, t_s, acc, sem):
        i = pl.program_id(0)

        def put(n, source, target):
            return pltpu.make_async_copy(source, target, sem.at[n])

        @pl.when(i == 0)
        def _():
            def body(rows):
                a = normed_block(x[rows, :].astype(F32))
                a_s[rows, :] = a
                t_s[:, rows] = a.T
                acc[rows, :] = jnp.zeros((TILE, D), F32)

            blocks(TOKENS, TILE, body)
            put(0, t_s, a1t).start()

        def body(rows):
            a = a_s[rows, :]
            g = dot(a, wg[...])
            u = dot(a, wu[...])
            gate[rows, :] = g
            up[rows, :] = u
            p = (g * lax.logistic(g) * u).astype(BF16)
            s[rows, :] = p
            acc[rows, :] += dot(p, wd[...])

        blocks(TOKENS, TOKENS, body)

        @pl.when(i == TILES - 1)
        def _():
            put(0, t_s, a1t).wait()

            def body(rows):
                h = x[rows, :] + acc[rows, :].astype(BF16)
                h_s[rows, :] = h
                a = normed_block(h.astype(F32))
                a_s[rows, :] = a
                t_s[:, rows] = a.T

            blocks(TOKENS, TILE, body)
            copies = [put(0, t_s, a2t), put(1, h_s, h1), put(2, a_s, a2)]
            for copy in copies:
                copy.start()
            for copy in copies:
                copy.wait()

    tokens, turned = jax.ShapeDtypeStruct((TOKENS, D), BF16), jax.ShapeDtypeStruct((D, TOKENS), BF16)
    hidden = (TOKENS, FF)
    return pl.pallas_call(
        kernel,
        grid=(TILES,),
        out_shape=[
            jax.ShapeDtypeStruct(hidden, F32),
            jax.ShapeDtypeStruct(hidden, F32),
            jax.ShapeDtypeStruct(hidden, BF16),
            turned,
            tokens,
            tokens,
            turned,
        ],
        in_specs=[kept((TOKENS, D)), wide_tile(0), wide_tile(0), deep_tile(0)],
        out_specs=[columns_tile()] * 3 + [ANY] * 4,
        scratch_shapes=[
            pltpu.VMEM((TOKENS, D), BF16),
            pltpu.VMEM((TOKENS, D), BF16),
            pltpu.VMEM((D, TOKENS), BF16),
            pltpu.VMEM((TOKENS, D), F32),
            pltpu.SemaphoreType.DMA((3,)),
        ],
        compiler_params=pltpu.CompilerParams(vmem_limit_bytes=VMEM_LIMIT),
        name="first_layer",
    )(x, w_gate, w_up, w_down)


def through_product(ds, g, u):
    sig = lax.logistic(g)
    silu = g * sig
    return (ds * u * (sig + silu * (1.0 - sig))).astype(BF16), (ds * silu).astype(BF16)


def second_layer(a2, dy, w_gate, w_up, w_down):
    def kernel(a2, dy, wg, wu, wd, dg, du, dwd, s):
        def body(rows):
            a = a2[rows, :]
            g = dot(a, wg[...])
            u = dot(a, wu[...])
            ds = dot(dy[rows, :], wd[...], NT).astype(BF16).astype(F32)
            s[rows, :] = (g * lax.logistic(g) * u).astype(BF16)
            dg[rows, :], du[rows, :] = through_product(ds, g, u)

        blocks(TOKENS, BLOCK, body)
        dwd[...] = dot(s[...], dy[...], TN).astype(BF16)

    return pl.pallas_call(
        kernel,
        grid=(TILES,),
        out_shape=[jax.ShapeDtypeStruct((TOKENS, FF), BF16)] * 2 + [jax.ShapeDtypeStruct((FF, D), BF16)],
        in_specs=[kept((TOKENS, D))] * 2 + [wide_tile(1), wide_tile(1), deep_tile(1)],
        out_specs=[columns_tile()] * 2 + [pl.BlockSpec((TILE, D), lambda i: (i, 0))],
        scratch_shapes=[pltpu.VMEM((TOKENS, TILE), BF16)],
        compiler_params=pltpu.CompilerParams(vmem_limit_bytes=VMEM_LIMIT),
        name="second_layer",
    )(a2, dy, w_gate, w_up, w_down)


def down_term(s, dh, gate, up, w_down):
    def kernel(s, dh, gate, up, wd, out, dg, du):
        def body(rows):
            ds = dot(dh[rows, :], wd[...], NT).astype(BF16).astype(F32)
            dg[rows, :], du[rows, :] = through_product(ds, gate[rows, :], up[rows, :])

        blocks(TOKENS, BLOCK, body)
        out[...] = dot(s[...], dh[...], TN).astype(BF16)

    return pl.pallas_call(
        kernel,
        grid=(TILES,),
        out_shape=[jax.ShapeDtypeStruct((FF, D), BF16)] + [jax.ShapeDtypeStruct((TOKENS, FF), BF16)] * 2,
        in_specs=[columns_tile(), kept((TOKENS, D)), columns_tile(), columns_tile(), deep_tile(0)],
        out_specs=[pl.BlockSpec((TILE, D), lambda i: (i, 0)), columns_tile(), columns_tile()],
        compiler_params=pltpu.CompilerParams(vmem_limit_bytes=VMEM_LIMIT),
        name="down_term",
    )(s, dh, gate, up, w_down)


def store_terms(at, dg, du, stage_g, stage_u):
    for stage, cotangent in ((stage_g, dg), (stage_u, du)):
        stage[...] = dot(at[...], cotangent[...]).astype(BF16).reshape(stage.shape)


class Terms:
    def __init__(self, stages, terms, sem):
        self.stages, self.terms, self.sem = stages, terms, sem

    def copies(self, tile):
        columns = pl.ds(pl.multiple_of(tile * TILE, TILE), TILE)
        return [
            pltpu.make_async_copy(stage, term.at[:, :, :, columns], self.sem.at[n])
            for n, (stage, term) in enumerate(zip(self.stages, self.terms, strict=True))
        ]

    def start(self, tile):
        for copy in self.copies(tile):
            copy.start()

    def wait(self, tile):
        for copy in self.copies(tile):
            copy.wait()


TERM = jax.ShapeDtypeStruct((4, 4, 64, FF), BF16)
STAGES = [pltpu.VMEM((4, 4, 64, TILE), BF16)] * 2 + [PAIR]


def second_sums(a2t, dg, du, w_gate, w_up, down, dy, h1, number):
    steps = 2 * TILES
    later = lambda begin: SECOND_LATE if begin >= 9 else SECOND_WIDE
    sums = Sums(
        (
            (DEEP, DOWN, (0,) * 6, lambda begin: SECOND_DOWN),
            (WIDE, GATE, READY, later),
            (WIDE, UP, READY, later),
        )
    )

    def kernel(a2t, dg, du, wg, wu, down, dy, h1, *refs):
        outs, refs = refs[:4], refs[4:]
        dh, term_g, term_u, stage_g, stage_u, term_sem, acc, half, half_sem, taken, taken_sem, *refs = refs
        i = pl.program_id(0)
        terms = Terms((stage_g, stage_u), (term_g, term_u), term_sem)
        enter, reach, rest = sums.run(i, steps, 1, (down, term_g, term_u), outs, refs)
        enter(NEXT)

        @pl.when((i > 0) & (i <= TILES))
        def _():
            terms.wait(i - 1)

        reach(0)

        @pl.when(i < TILES)
        def _():
            store_terms(a2t, dg, du, stage_g, stage_u)
            terms.start(i)

        @pl.when(i == TILES)
        def _():
            blocks(TOKENS, TILE, lambda rows: acc.__setitem__((rows, slice(None)), jnp.zeros((TILE, D), F32)))

        @pl.when(i >= TILES)
        def _():
            def body(rows):
                acc[rows, :] += dot(dg[rows, :], wg[...], NT) + dot(du[rows, :], wu[...], NT)

            blocks(TOKENS, TOKENS, body)

        def take(n):
            rows = pl.ds(PART * n, PART)
            return [
                pltpu.make_async_copy(source.at[rows, :], taken.at[n % 2, which], taken_sem.at[n % 2, which])
                for which, source in enumerate((dy, h1))
            ]

        def give(n):
            return pltpu.make_async_copy(half.at[n % 2], dh.at[pl.ds(PART * n, PART), :], half_sem.at[n % 2])

        @pl.when(i == steps - 1)
        def _():
            parts = TOKENS // PART
            for copy in take(0):
                copy.start()
            for n in range(parts):
                if n + 1 < parts:
                    for copy in take(n + 1):
                        copy.start()
                for copy in take(n):
                    copy.wait()
                if n >= 2:
                    give(n - 2).wait()

                def body(rows, n=n):
                    da = acc[pl.ds(pl.multiple_of(PART * n + rows.start, 8), rows.size), :].astype(BF16)
                    half[n % 2, rows, :] = through_norm(taken[n % 2, 0, rows, :], da, taken[n % 2, 1, rows, :])

                blocks(PART, PART, body)
                give(n).start()
            give(parts - 2).wait()
            give(parts - 1).wait()

        rest()

    turn = lambda i: lax.rem(i, TILES)
    late = lambda i: jnp.maximum(i - TILES, 0)
    d, g, u, squares, dh, *_ = pl.pallas_call(
        kernel,
        grid=(steps,),
        out_shape=[*sums.out_shape, jax.ShapeDtypeStruct((TOKENS, D), BF16), TERM, TERM],
        in_specs=[kept((D, TOKENS)), columns_tile(turn), columns_tile(turn), wide_tile(1, late), wide_tile(1, late), ANY, ANY, ANY],
        out_specs=[VMEM] * 4 + [ANY] * 3,
        scratch_shapes=[
            *STAGES,
            pltpu.VMEM((TOKENS, D), F32),
            pltpu.VMEM((2, PART, D), BF16),
            PAIR,
            pltpu.VMEM((2, 2, PART, D), BF16),
            pltpu.SemaphoreType.DMA((2, 2)),
            *sums.scratch_shapes,
        ],
        compiler_params=pltpu.CompilerParams(collective_id=number, has_side_effects=True, vmem_limit_bytes=VMEM_LIMIT),
        name="second_sums",
    )(a2t, dg, du, w_gate, w_up, down.reshape(4, 4, 176, D), dy, h1)
    return d, g, u, squares, dh


def first_sums(a1t, dg, du, down, others, number):
    steps = TILES
    sums = Sums(
        (
            (DEEP, DOWN, (0,) * 6, lambda begin: FIRST_DOWN),
            (WIDE, GATE, READY, lambda begin: FIRST_WIDE),
            (WIDE, UP, READY, lambda begin: FIRST_WIDE),
        )
    )

    def kernel(a1t, dg, du, down, others, *refs):
        outs, refs = refs[:4], refs[4:]
        total, term_g, term_u, stage_g, stage_u, term_sem, *refs = refs
        *refs, got, held, norm_send, norm_recv = refs
        i = pl.program_id(0)
        terms = Terms((stage_g, stage_u), (term_g, term_u), term_sem)
        enter, reach, rest = sums.run(i, steps, 1, (down, term_g, term_u), outs, refs)
        enter([(axis, by) for axis in AXES for by in AROUND])

        @pl.when(i > 0)
        def _():
            terms.wait(i - 1)

        reach(0)

        store_terms(a1t, dg, du, stage_g, stage_u)
        terms.start(i)

        @pl.when(i == steps - 1)
        def _():
            terms.wait(i)

        rest()

        @pl.when(i == steps - 1)
        def _():
            norm(jnp.sum(outs[3][...] + others[...]), total, got, held, norm_send, norm_recv)

    d, g, u, _, total, *_ = pl.pallas_call(
        kernel,
        grid=(steps,),
        out_shape=[*sums.out_shape, jax.ShapeDtypeStruct(SCALAR, F32), TERM, TERM],
        in_specs=[kept((D, TOKENS)), columns_tile(), columns_tile(), ANY, VMEM],
        out_specs=[VMEM] * 5 + [ANY] * 2,
        scratch_shapes=[*STAGES, *sums.scratch_shapes, *NORM],
        compiler_params=pltpu.CompilerParams(collective_id=number, has_side_effects=True, vmem_limit_bytes=VMEM_LIMIT),
        name="first_sums",
    )(a1t, dg, du, down.reshape(4, 4, 176, D), others)
    return d, g, u, total


AROUND = (1, -1, 2)
SCALAR = (8, 128)
NORM = [
    pltpu.VMEM((3, 3, *SCALAR), F32),
    pltpu.VMEM((4, *SCALAR), F32),
    pltpu.SemaphoreType.DMA((3, 3)),
    pltpu.SemaphoreType.DMA((3, 3)),
]


def norm(own, out, got, held, send, recv):
    held[0] = jnp.full(SCALAR, own, F32)
    for axis in AXES:
        copies = [
            pltpu.make_async_remote_copy(
                src_ref=held.at[axis],
                dst_ref=got.at[axis, n],
                send_sem=send.at[axis, n],
                recv_sem=recv.at[axis, n],
                device_id=at(axis, by),
                device_id_type=MESH,
            )
            for n, by in enumerate(AROUND)
        ]
        for copy in copies:
            copy.start()
        for copy in copies:
            copy.wait_recv()
        held[axis + 1] = (held[axis] + got[axis, 2]) + (got[axis, 0] + got[axis, 1])
        for copy in copies:
            copy.wait_send()
    out[...] = held[3]


class GatherJob:
    def __init__(self, form, colour, remote, local):
        self.form = form
        self.colour, self.first, self.width = colour
        self.axes = [(self.colour + n) % 3 for n in AXES]
        self.numbers = [[remote.new() for _ in range(4)] for _ in AXES]
        self.local_number = local.new()

    def bind(self, own, out, send, recv, local):
        self.own, self.out, self.send, self.recv, self.local = own, out, send, recv, local

    def held(self, n, by, layer=None):
        index = []
        for axis in AXES:
            if axis in self.axes[:n]:
                index.append(slice(None))
                continue
            k = place(axis, by if axis == self.axes[n] else 0)
            window = WINDOW[self.form]
            index.append(pl.ds(pl.multiple_of(k * window, 8), window) if axis == 2 else pl.ds(k, 1))
        layers = slice(None) if layer is None else pl.ds(layer, 1)
        return self.out.at[(layers, *index, pl.ds(self.first, self.width))]

    def copy(self, n, which):
        axis, number = self.axes[n], self.numbers[n][which]
        if which < 2:
            by = (1, -1)[which]
            source = self.own.at[:, :, :, :, pl.ds(self.first, self.width)] if n == 0 else self.held(n, 0)
            target = self.held(n, 0)
        else:
            by = (1, -1)[which - 2]
            source = target = self.held(n, -by, which - 2)
        return pltpu.make_async_remote_copy(
            src_ref=source,
            dst_ref=target,
            send_sem=self.send.at[number],
            recv_sem=self.recv.at[number],
            device_id=at(axis, by),
            device_id_type=MESH,
        )

    def keep(self):
        return pltpu.make_async_copy(
            self.own.at[:, :, :, :, pl.ds(self.first, self.width)], self.held(0, 0), self.local.at[self.local_number]
        )

    def actions(self):
        for n in AXES:

            def begin(n=n):
                if n == 0:
                    self.keep().start()
                else:
                    self.copy(n - 1, 2).wait_recv()
                    self.copy(n - 1, 3).wait_recv()
                if n == 1:
                    self.keep().wait()
                self.copy(n, 0).start()
                self.copy(n, 1).start()

            def forward(n=n):
                self.copy(n, 0).wait_recv()
                self.copy(n, 2).start()
                self.copy(n, 1).wait_recv()
                self.copy(n, 3).start()

            yield begin
            yield forward

        def last():
            self.copy(2, 2).wait_recv()
            self.copy(2, 3).wait_recv()
            for n in AXES:
                for which in range(4):
                    self.copy(n, which).wait_send()

        yield last


def close_up(padded, closed, rows):
    def step(t, _):
        layer, pair = lax.div(t, 16), lax.rem(t, 16)
        for z in range(4):
            block = padded[layer, lax.div(pair, 4), lax.rem(pair, 4), pl.ds(48 * z, 48), :]
            rows[pl.ds(44 * z, 48), :] = block.astype(F32)
        closed[layer, pair] = rows[pl.ds(0, 176), :].astype(BF16)
        return 0

    lax.fori_loop(0, 32, step, 0)


def gather_kernel(forms, number):
    shapes = [(2, 4, 4, 4 * WINDOW[f], COLUMNS[f]) for f in forms]
    remote, local = Copies(), Copies()
    jobs = [[GatherJob(form, colour, remote, local) for colour in COLOURS[form]] for form in forms]

    def kernel(*refs):
        owns, (*outs, closed) = refs[: len(forms)], refs[len(forms) : 2 * len(forms)]
        padded, rows, send, recv, loc = refs[2 * len(forms) :]
        outs.append(padded)
        greet(NEXT)
        order = []
        for m, of_matrix in enumerate(jobs):
            for j, job in enumerate(of_matrix):
                job.bind(owns[m], outs[m], send, recv, loc)
                for stage, action in enumerate(job.actions()):
                    order.append((stage if forms[m] == DEEP else stage + 1.5, m, j, action))
        order.append((6.2, 0, 0, lambda: close_up(padded, closed, rows)))
        for *_, action in sorted(order, key=lambda o: o[:3]):
            action()

    def call(*owns):
        return pl.pallas_call(
            kernel,
            out_shape=[pltpu.VMEM(s, BF16) for s in (*shapes[:-1], (2, 16, 176, D))],
            in_specs=[VMEM] * len(forms),
            out_specs=[VMEM] * len(forms),
            scratch_shapes=[
                pltpu.VMEM(shapes[-1], BF16),
                pltpu.VMEM((184, D), F32),
                pltpu.SemaphoreType.DMA((remote.count,)),
                pltpu.SemaphoreType.DMA((remote.count,)),
                pltpu.SemaphoreType.DMA((local.count,)),
            ],
            compiler_params=pltpu.CompilerParams(collective_id=number, has_side_effects=True, vmem_limit_bytes=2 * SMALL_LIMIT),
            name="gather",
        )(*(o.reshape(2, 1, 1, WINDOW[f], COLUMNS[f]) for o, f in zip(owns, forms, strict=True)))

    return call


def settle(*weights):
    def kernel(*refs):
        sem = refs[-1]
        copies = [
            pltpu.make_async_copy(refs[n].at[layer], refs[3 + n].at[layer], sem.at[n, layer]) for n in AXES for layer in (0, 1)
        ]
        for copy in copies:
            copy.start()
        for copy in copies:
            copy.wait()

    return pl.pallas_call(
        kernel,
        out_shape=[jax.ShapeDtypeStruct(w.shape, BF16) for w in weights],
        in_specs=[VMEM] * 3,
        out_specs=[ANY] * 3,
        scratch_shapes=[pltpu.SemaphoreType.DMA((3, 2))],
        compiler_params=pltpu.CompilerParams(vmem_limit_bytes=SMALL_LIMIT),
        name="settle",
    )(*weights)


def through_norm(dy, da, h):
    wide, da = h.astype(F32), da.astype(F32)
    scale = lax.rsqrt(jnp.mean(wide**2, -1, keepdims=True) + 1e-6)
    along = jnp.mean(da * wide, -1, keepdims=True) * scale**3
    return dy + (da * scale - wide * along).astype(BF16)


def adamw(w, m, v, g):
    m = 0.9 * m + 0.1 * g
    v = 0.95 * v + 0.05 * g * g
    step = m * lax.rsqrt(v + 1e-8) + 0.1 * w
    return (w - 0.02 * step).astype(BF16), m, v


def solution(mesh):
    def step(x, dy, *arrays):
        weights, m, v = (arrays[i : i + 3] for i in (0, 3, 6))
        x, dy = x[0], dy[0]
        w_gate, w_up, w_down = weights
        z = lax.rem(lax.axis_index("dp"), 4)
        gate1, up1, s1, a1t, h1, a2, a2t = first_layer(x, w_gate, w_up, w_down)
        dg, du, down2 = second_layer(a2, dy, w_gate, w_up, w_down)
        down_2, gate_2, up_2, squares_2, dh = second_sums(a2t, dg, du, w_gate, w_up, down2, dy, h1, 0)
        down1, dg, du = down_term(s1, dh, gate1, up1, w_down)
        down_1, gate_1, up_1, total = first_sums(a1t, dg, du, down1, squares_2, 1)
        gate, up = (gate_1, gate_2), (up_1, up_2)
        down = [lax.dynamic_slice_in_dim(d, 4 * lax.rem(z, 2), 44, 0) for d in (down_1, down_2)]
        gradients = [jnp.stack(g).astype(F32) for g in (gate, up, down)]
        factor = jnp.minimum(1.0, 0.5 * lax.rsqrt(total[0, 0] / (6 * D * FF) + 1e-30))
        new = []
        for w, m_, v_, g in zip(weights, m, v, gradients, strict=True):
            rows = g.shape[1]
            own = lax.dynamic_slice_in_dim(w, lax.axis_index("dp") * rows, rows, 1)
            new.append(adamw(own.astype(F32), m_, v_, g * factor))
        own = [one[0] for one in new]
        own[2] = jnp.pad(own[2], ((0, 0), (0, 4), (0, 0)))
        gate, up, down = settle(*gather_kernel((WIDE, WIDE, DEEP), 2)(*own))
        return (
            gate.reshape(2, D, FF),
            up.reshape(2, D, FF),
            down.reshape(2, FF, D),
            *(one[1] for one in new),
            *(one[2] for one in new),
        )

    whole, rows = P(None, None, None), P(None, "dp", None)
    tokens, out, out_rows = P(("rep", "dp"), None, None), P("rep", None, None), P("rep", "dp", None)
    return jax.shard_map(
        step,
        mesh=mesh,
        in_specs=(tokens, tokens, *[whole] * 3, *[rows] * 6),
        out_specs=(*[out] * 3, *[out_rows] * 6),
        check_vma=False,
    )
```
